16 devices in a mesh: rep: 2 (over y, z), dp: 8 (over x, core).
Axes of the slice: x: 4, y: 2, z: 1, core: 2. Of those that a mesh axis runs over, the one named last changes fastest.
The devices are a block of a 4x4x8 slice.
Arguments:
- x: bfloat16 [16, 2048, 640], P(('rep', 'dp')), parts along dimension 0
- dy: bfloat16 [16, 2048, 640], P(('rep', 'dp')), parts along dimension 0
- w_gate: bfloat16 [2, 640, 3456], replicated
- w_up: bfloat16 [2, 640, 3456], replicated
- w_down: bfloat16 [2, 3456, 640], replicated
- m_w_gate: float32 [2, 640, 3456], replicated
- m_w_up: float32 [2, 640, 3456], replicated
- m_w_down: float32 [2, 3456, 640], replicated
- v_w_gate: float32 [2, 640, 3456], replicated
- v_w_up: float32 [2, 640, 3456], replicated
- v_w_down: float32 [2, 3456, 640], replicated
Outputs:
- output 1: bfloat16 [4, 640, 3456], P('rep'), parts along dimension 0
- output 2: bfloat16 [4, 640, 3456], P('rep'), parts along dimension 0
- output 3: bfloat16 [4, 3456, 640], P('rep'), parts along dimension 0
- output 4: float32 [4, 640, 3456], P('rep'), parts along dimension 0
- output 5: float32 [4, 640, 3456], P('rep'), parts along dimension 0
- output 6: float32 [4, 3456, 640], P('rep'), parts along dimension 0
- output 7: float32 [4, 640, 3456], P('rep'), parts along dimension 0
- output 8: float32 [4, 640, 3456], P('rep'), parts along dimension 0
- output 9: float32 [4, 3456, 640], P('rep'), parts along dimension 0
There are 2 independent parts. The reference program is written for one: setup_inputs(seed, part) draws one part's arguments, and reference() takes and returns one part's arrays. A program takes and returns all parts, laid end to end along the dimension named above; an argument that names none is the same for every part.
All inputs are finite; a program needn't handle non-finite values.
Results may differ from the reference program's by a relative error of at most 0.022.
Values are sent between devices in bfloat16 or wider.
A program may use at most 768 MiB of HBM per device.

```python
import jax
import jax.numpy as jnp
from jax import lax

SEQUENCES = 8
TOKENS = 2048
D = 640
FF = 3456
LAYERS = 2
NAMES = ("w_gate", "w_up", "w_down")
SHAPES = {"w_gate": (LAYERS, D, FF), "w_up": (LAYERS, D, FF), "w_down": (LAYERS, FF, D)}


def bump(key, n, height):
    away = (jnp.arange(n, dtype=jnp.int32) - jax.random.randint(key, (), 0, n, jnp.int32)) % n
    return jnp.where(away < n // 8, height, 1.0)


def together(key, own, strength):
    shared = jax.random.normal(key, own.shape[1:], jnp.float32)
    return (own + strength * shared) * lax.rsqrt(1 + strength * strength)


def setup_inputs(seed: int = 0, part: int = 0) -> dict:
    kx, kdy, ka, kb, kz, kf, kh, kl, *keys = jax.random.split(jax.random.key(seed), 8 + 3 * len(NAMES))
    kx, kdy, ka, kb = (jax.random.fold_in(k, part) for k in (kx, kdy, ka, kb))
    kw, km, kv = (keys[i::3] for i in range(3))
    shape = (SEQUENCES, TOKENS, D)
    much_x, much_dy = jax.random.uniform(kz, (2,), jnp.float32, 0.0, 1.0)
    loud = 2.0 ** jax.random.uniform(jax.random.fold_in(kz, 1), (), jnp.float32, -1.0, 2.0)
    layers = 2.0 ** jax.random.uniform(kl, (LAYERS, 1, 1), jnp.float32, -1.0, 1.0)
    x = together(ka, jax.random.normal(kx, shape, jnp.float32), much_x) * bump(kf, D, 4.0)
    dy = together(kb, jax.random.normal(kdy, shape, jnp.float32), much_dy)
    drawn = {"x": x.astype(jnp.bfloat16), "dy": (loud * dy * (SEQUENCES * TOKENS) ** -0.5).astype(jnp.bfloat16)}
    for key, name in zip(kw, NAMES, strict=True):
        w = jax.random.normal(key, SHAPES[name], jnp.float32) * SHAPES[name][1] ** -0.5
        drawn[name] = (w * {"w_gate": 1.0, "w_up": bump(kh, FF, 4.0), "w_down": layers}[name]).astype(jnp.bfloat16)
    for key, name in zip(km, NAMES, strict=True):
        drawn[f"m_{name}"] = 0.1 * jax.random.normal(key, SHAPES[name], jnp.float32)
    for key, name in zip(kv, NAMES, strict=True):
        drawn[f"v_{name}"] = jax.random.uniform(key, SHAPES[name], jnp.float32, 0.005, 0.015)
    return drawn


def matmul(a, w):
    return jnp.dot(a, w, preferred_element_type=jnp.float32).astype(jnp.bfloat16)


def normed(h):
    wide = h.astype(jnp.float32)
    scale = lax.rsqrt(jnp.mean(wide**2, -1, keepdims=True) + 1e-6)
    return (wide * scale).astype(jnp.bfloat16)


def layer(h, w):
    a = normed(h)
    gate = jnp.dot(a, w["w_gate"], preferred_element_type=jnp.float32)
    up = jnp.dot(a, w["w_up"], preferred_element_type=jnp.float32)
    return h + matmul((jax.nn.silu(gate) * up).astype(jnp.bfloat16), w["w_down"])


def adamw(w, m, v, g):
    m = 0.9 * m + 0.1 * g
    v = 0.95 * v + 0.05 * g * g
    step = m * lax.rsqrt(v + 1e-8) + 0.1 * w
    return (w - 0.02 * step).astype(jnp.bfloat16), m, v


def clipped(gradients, sum_of_squares, count):
    factor = jnp.minimum(1.0, 0.5 * lax.rsqrt(sum_of_squares / count + 1e-30))
    return [g * factor for g in gradients]


def stack(weights, h):
    return lax.scan(lambda h, w: (layer(h, w), None), h, weights)[0]


def reference(x, dy, w_gate, w_up, w_down, m_w_gate, m_w_up, m_w_down, v_w_gate, v_w_up, v_w_down):
    weights = dict(zip(NAMES, (w_gate, w_up, w_down), strict=True))

    def take(so_far, sequence):
        h, by_y = sequence
        _, back = jax.vjp(lambda w: stack(w, h), weights)
        return jax.tree.map(lambda total, term: total + term.astype(jnp.float32), so_far, back(by_y)[0]), None

    none_yet = {name: jnp.zeros(w.shape, jnp.float32) for name, w in weights.items()}
    by_weights, _ = lax.scan(take, none_yet, (x, dy))
    gradients = [by_weights[name].astype(jnp.bfloat16).astype(jnp.float32) for name in NAMES]
    gradients = clipped(gradients, sum(jnp.sum(g * g) for g in gradients), sum(g.size for g in gradients))
    new = [
        adamw(w.astype(jnp.float32), m, v, g)
        for w, m, v, g in zip((w_gate, w_up, w_down), (m_w_gate, m_w_up, m_w_down), (v_w_gate, v_w_up, v_w_down), gradients, strict=True)
    ]
    return tuple(one[which] for which in range(3) for one in new)
```

```python
import functools
import jax
import jax.numpy as jnp
from jax import lax
from jax.experimental import pallas as pl
from jax.experimental.pallas import tpu as pltpu

F32, BF16 = jnp.float32, jnp.bfloat16
TILE = 512
CHUNK = 256


def nn(a, b):
    return jnp.dot(a, b, preferred_element_type=F32)


def nt(a, b):
    return lax.dot_general(a, b, (((1,), (1,)), ((), ())), preferred_element_type=F32)


def scale_of(wide):
    return lax.rsqrt(jnp.mean(wide * wide, -1, keepdims=True) + 1e-6)


def sigmoid(x):
    return 0.5 * jnp.tanh(0.5 * x) + 0.5


def rows_of(c):
    return pl.ds(pl.multiple_of(c * CHUNK, CHUNK), CHUNK)


def hold(ref, kept, axis, left):
    kept[...] = ref[0]
    if left < TILE:
        @pl.when(pl.program_id(0) == pl.num_programs(0) - 1)
        def _():
            if axis == 1:
                kept[:, left:] = jnp.zeros((kept.shape[0], TILE - left), kept.dtype)
            else:
                kept[left:, :] = jnp.zeros((TILE - left, kept.shape[1]), kept.dtype)


def forward_kernel(chunks, left, x_ref, wg_ref, wu_ref, wd_ref, h_ref, gate_ref, up_ref, a, acc, wg, wu, wd):
    j = pl.program_id(0)

    @pl.when(j == 0)
    def _():
        def norm(c, _):
            wide = x_ref[rows_of(c), :].astype(F32)
            a[rows_of(c), :] = (wide * scale_of(wide)).astype(BF16)
            acc[rows_of(c), :] = jnp.zeros((CHUNK, acc.shape[1]), F32)
            return _
        lax.fori_loop(0, chunks, norm, 0)

    hold(wg_ref, wg, 1, left)
    hold(wu_ref, wu, 1, left)
    hold(wd_ref, wd, 0, left)

    def body(c, _):
        r = rows_of(c)
        gate = nn(a[r, :], wg[...])
        up = nn(a[r, :], wu[...])
        gate_ref[r, :] = gate
        up_ref[r, :] = up
        act = (gate * sigmoid(gate) * up).astype(BF16)
        acc[r, :] += nn(act, wd[...])
        return _
    lax.fori_loop(0, chunks, body, 0)

    @pl.when(j == pl.num_programs(0) - 1)
    def _():
        def out(c, _):
            r = rows_of(c)
            h_ref[r, :] = (x_ref[r, :].astype(F32) + acc[r, :].astype(BF16).astype(F32)).astype(BF16)
            return _
        lax.fori_loop(0, chunks, out, 0)


def backward_kernel(chunks, left, last_layer, *refs):
    if last_layer:
        h_ref, dy_ref, wg_ref, wu_ref, wd_ref, g_ref, dh_ref, a, at, dyt, act, dgate, dup, acc, wg, wu, wd = refs
    else:
        h_ref, dy_ref, gate_ref, up_ref, wd_ref, g_ref, at, dyt, act, dgate, dup, wd = refs
    j = pl.program_id(0)

    @pl.when(j == 0)
    def _():
        def norm(c, _):
            r = rows_of(c)
            wide = h_ref[r, :].astype(F32)
            normed = (wide * scale_of(wide)).astype(BF16)
            at[:, r] = normed.T
            dyt[:, r] = dy_ref[r, :].T
            if last_layer:
                a[r, :] = normed
                acc[r, :] = jnp.zeros((CHUNK, acc.shape[1]), F32)
            return _
        lax.fori_loop(0, chunks, norm, 0)

    if last_layer:
        hold(wg_ref, wg, 1, left)
        hold(wu_ref, wu, 1, left)
    hold(wd_ref, wd, 0, left)

    def body(c, _):
        r = rows_of(c)
        if last_layer:
            gate = nn(a[r, :], wg[...])
            up = nn(a[r, :], wu[...])
        else:
            gate = gate_ref[r, :]
            up = up_ref[r, :]
        d = nt(dy_ref[r, :], wd[...]).astype(BF16).astype(F32)
        s = sigmoid(gate)
        silu = gate * s
        act[r, :] = (silu * up).astype(BF16)
        d_up = (d * silu).astype(BF16)
        d_gate = (d * up * (s + silu * (1.0 - s))).astype(BF16)
        dup[r, :] = d_up
        dgate[r, :] = d_gate
        if last_layer:
            acc[r, :] += nt(d_gate, wg[...]) + nt(d_up, wu[...])
        return _
    lax.fori_loop(0, chunks, body, 0)

    g_ref[:, 0:TILE] = nn(at[...], dgate[...]).astype(BF16)
    g_ref[:, TILE : 2 * TILE] = nn(at[...], dup[...]).astype(BF16)
    g_ref[:, 2 * TILE : 3 * TILE] = nn(dyt[...], act[...]).astype(BF16)

    if last_layer:
        @pl.when(j == pl.num_programs(0) - 1)
        def _():
            def out(c, _):
                r = rows_of(c)
                wide = h_ref[r, :].astype(F32)
                scale = scale_of(wide)
                da = acc[r, :].astype(BF16).astype(F32)
                dot = jnp.mean(da * wide, -1, keepdims=True)
                by = scale * da - wide * (scale * scale * scale * dot)
                dh_ref[r, :] = (dy_ref[r, :].astype(F32) + by.astype(BF16).astype(F32)).astype(BF16)
                return _
            lax.fori_loop(0, chunks, out, 0)


def whole(shape):
    return pl.BlockSpec(shape, lambda j: (0,) * len(shape))


def params():
    return pltpu.CompilerParams(dimension_semantics=("arbitrary",), vmem_limit_bytes=62 * 1024 * 1024)


def forward(x, w, layer):
    tokens, d = x.shape
    ff = w[0].shape[2]
    tiles = pl.cdiv(ff, TILE)
    col = pl.BlockSpec((1, d, TILE), lambda j: (layer, 0, j))
    row = pl.BlockSpec((1, TILE, d), lambda j: (layer, j, 0))
    saved = pl.BlockSpec((tokens, TILE), lambda j: (0, j))
    return pl.pallas_call(
        functools.partial(forward_kernel, tokens // CHUNK, ff - (tiles - 1) * TILE),
        grid=(tiles,),
        in_specs=[whole((tokens, d)), col, col, row],
        out_specs=[whole((tokens, d)), saved, saved],
        out_shape=[jax.ShapeDtypeStruct((tokens, d), BF16)] + [jax.ShapeDtypeStruct((tokens, tiles * TILE), F32)] * 2,
        scratch_shapes=[pltpu.VMEM((tokens, d), BF16), pltpu.VMEM((tokens, d), F32), pltpu.VMEM((d, TILE), BF16), pltpu.VMEM((d, TILE), BF16), pltpu.VMEM((TILE, d), BF16)],
        compiler_params=params(),
        cost_estimate=pl.CostEstimate(flops=6 * tokens * d * ff, bytes_accessed=8 * tokens * ff, transcendentals=tokens * ff),
        name="forward",
    )(x, *w)


def backward_last(h, dy, w, layer):
    tokens, d = h.shape
    ff = w[0].shape[2]
    tiles = pl.cdiv(ff, TILE)
    col = pl.BlockSpec((1, d, TILE), lambda j: (layer, 0, j))
    row = pl.BlockSpec((1, TILE, d), lambda j: (layer, j, 0))
    return pl.pallas_call(
        functools.partial(backward_kernel, tokens // CHUNK, ff - (tiles - 1) * TILE, True),
        grid=(tiles,),
        in_specs=[whole((tokens, d)), whole((tokens, d)), col, col, row],
        out_specs=[pl.BlockSpec((d, 3 * TILE), lambda j: (0, j)), whole((tokens, d))],
        out_shape=[jax.ShapeDtypeStruct((d, 3 * TILE * tiles), BF16), jax.ShapeDtypeStruct((tokens, d), BF16)],
        scratch_shapes=[pltpu.VMEM((tokens, d), BF16)] + [pltpu.VMEM((d, tokens), BF16)] * 2 + [pltpu.VMEM((tokens, TILE), BF16)] * 3
        + [pltpu.VMEM((tokens, d), F32), pltpu.VMEM((d, TILE), BF16), pltpu.VMEM((d, TILE), BF16), pltpu.VMEM((TILE, d), BF16)],
        compiler_params=params(),
        cost_estimate=pl.CostEstimate(flops=16 * tokens * d * ff, bytes_accessed=12 * d * ff, transcendentals=tokens * ff),
        name="backward_last",
    )(h, dy, *w)


def backward_first(h, dy, gate, up, wd, layer):
    tokens, d = h.shape
    ff = wd.shape[1]
    tiles = pl.cdiv(ff, TILE)
    row = pl.BlockSpec((1, TILE, d), lambda j: (layer, j, 0))
    saved = pl.BlockSpec((tokens, TILE), lambda j: (0, j))
    return pl.pallas_call(
        functools.partial(backward_kernel, tokens // CHUNK, ff - (tiles - 1) * TILE, False),
        grid=(tiles,),
        in_specs=[whole((tokens, d)), whole((tokens, d)), saved, saved, row],
        out_specs=pl.BlockSpec((d, 3 * TILE), lambda j: (0, j)),
        out_shape=jax.ShapeDtypeStruct((d, 3 * TILE * tiles), BF16),
        scratch_shapes=[pltpu.VMEM((d, tokens), BF16)] * 2 + [pltpu.VMEM((tokens, TILE), BF16)] * 3 + [pltpu.VMEM((TILE, d), BF16)],
        compiler_params=params(),
        cost_estimate=pl.CostEstimate(flops=8 * tokens * d * ff, bytes_accessed=8 * tokens * ff, transcendentals=tokens * ff),
        name="backward_first",
    )(h, dy, gate, up, wd)


def adamw_kernel(fresh, factor_ref, g_ref, *refs):
    w_refs, m_refs, v_refs = refs[0:3], refs[3:6], refs[6:9]
    outs = refs[9:] if fresh else refs[18:]
    factor = factor_ref[0, 0]
    for i in range(3):
        g = g_ref[:, i * TILE : (i + 1) * TILE].astype(F32) * factor
        if i == 2:
            g = g.T
        m = 0.9 * m_refs[i][0] + 0.1 * g
        v = 0.95 * v_refs[i][0] + 0.05 * g * g
        w = w_refs[i][0].astype(F32)
        outs[i][0] = (w - 0.02 * (m * lax.rsqrt(v + 1e-8) + 0.1 * w)).astype(BF16)
        outs[3 + i][0] = m
        outs[6 + i][0] = v


def adamw(factor, g, w, m, v, layer, so_far=None):
    layers, d, ff = w[0].shape
    tiles = pl.cdiv(ff, TILE)
    col = pl.BlockSpec((1, d, TILE), lambda j: (layer, 0, j))
    row = pl.BlockSpec((1, TILE, d), lambda j: (layer, j, 0))
    nine = [col, col, row] * 3
    arrays = [*w, *m, *v]
    held = [] if so_far is None else list(so_far)
    return pl.pallas_call(
        functools.partial(adamw_kernel, so_far is None),
        grid=(tiles,),
        in_specs=[pl.BlockSpec(memory_space=pltpu.SMEM), pl.BlockSpec((d, 3 * TILE), lambda j: (0, j))] + nine + [pl.BlockSpec(memory_space=pl.ANY)] * len(held),
        out_specs=nine,
        out_shape=[jax.ShapeDtypeStruct(a.shape, a.dtype) for a in arrays],
        input_output_aliases={11 + i: i for i in range(len(held))},
        compiler_params=params(),
        cost_estimate=pl.CostEstimate(flops=60 * d * ff, bytes_accessed=66 * d * ff, transcendentals=3 * d * ff),
        name="adamw",
    )(factor, g, *arrays, *held)


def solution(mesh):
    from jax.sharding import PartitionSpec as P

    def step(x, dy, *arrays):
        w, m, v = (arrays[i : i + 3] for i in (0, 3, 6))
        x, dy = x[0], dy[0]
        h, gate, up = forward(x, w, 0)
        g1, dh = backward_last(h, dy, w, 1)
        s1 = lax.psum_scatter(g1, "dp", scatter_dimension=0, tiled=True)
        g0 = backward_first(x, dh, gate, up, w[2], 0)
        s0 = lax.psum_scatter(g0, "dp", scatter_dimension=0, tiled=True)
        squares = sum(jnp.sum(s.astype(F32) ** 2) for s in (s1, s0))
        squares = lax.psum(squares, "dp")
        count = sum(a.size for a in w)
        factor = jnp.minimum(1.0, 0.5 * lax.rsqrt(squares / count + 1e-30)).reshape(1, 1)
        t1 = lax.all_gather(s1, "dp", axis=0, tiled=True)
        t0 = lax.all_gather(s0, "dp", axis=0, tiled=True)
        new = adamw(factor, t1, w, m, v, 1)
        return tuple(adamw(factor, t0, w, m, v, 0, new))

    return jax.shard_map(
        step,
        mesh=mesh,
        in_specs=(P(("rep", "dp"), None, None),) * 2 + (P(None, None, None),) * 9,
        out_specs=(P("rep", None, None),) * 9,
        check_vma=False,
    )
```

```python
import functools
import jax
import jax.numpy as jnp
from jax import lax
from jax.experimental import pallas as pl
from jax.experimental.pallas import tpu as pltpu
from jax.sharding import PartitionSpec as P

F32, BF16 = jnp.float32, jnp.bfloat16
TILE = 512
CHUNK = 1024
WIDE = 2048
SLOTS, HALF_SLOTS, RING_SLOTS = 4, 6, 3
MESH = pl.DeviceIdType.MESH


def nn(a, b):
    return jnp.dot(a, b, preferred_element_type=F32)


def nt(a, b):
    return lax.dot_general(a, b, (((1,), (1,)), ((), ())), preferred_element_type=F32)


def scale_of(wide):
    return lax.rsqrt(jnp.mean(wide * wide, -1, keepdims=True) + 1e-6)


def sigmoid(x):
    return 0.5 * jnp.tanh(0.5 * x) + 0.5


def rows_of(c):
    return pl.ds(pl.multiple_of(c * CHUNK, CHUNK), CHUNK)


def hold(ref, kept, axis, left, at_end):
    kept[...] = ref[0]
    if left < TILE:
        @pl.when(at_end)
        def _():
            if axis == 1:
                kept[:, left:] = jnp.zeros((kept.shape[0], TILE - left), kept.dtype)
            else:
                kept[left:, :] = jnp.zeros((TILE - left, kept.shape[1]), kept.dtype)


def forward_kernel(chunks, left, x_ref, wg_ref, wu_ref, wd_ref, h_ref, at_ref, gate_ref, up_ref, a, acc, wg, wu, wd):
    j = pl.program_id(0)

    @pl.when(j == 0)
    def _():
        def norm(c, _):
            wide = x_ref[rows_of(c), :].astype(F32)
            normed = (wide * scale_of(wide)).astype(BF16)
            a[rows_of(c), :] = normed
            at_ref[:, rows_of(c)] = normed.T
            acc[rows_of(c), :] = jnp.zeros((CHUNK, acc.shape[1]), F32)
            return _
        lax.fori_loop(0, chunks, norm, 0)

    hold(wg_ref, wg, 1, left, j == pl.num_programs(0) - 1)
    hold(wu_ref, wu, 1, left, j == pl.num_programs(0) - 1)
    hold(wd_ref, wd, 0, left, j == pl.num_programs(0) - 1)

    def body(c, _):
        r = rows_of(c)
        gate = nn(a[r, :], wg[...])
        up = nn(a[r, :], wu[...])
        gate_ref[r, :] = gate
        up_ref[r, :] = up
        act = (gate * sigmoid(gate) * up).astype(BF16)
        acc[r, :] += nn(act, wd[...])
        return _
    lax.fori_loop(0, chunks, body, 0)

    @pl.when(j == pl.num_programs(0) - 1)
    def _():
        def out(c, _):
            r = rows_of(c)
            h_ref[r, :] = (x_ref[r, :].astype(F32) + acc[r, :].astype(BF16).astype(F32)).astype(BF16)
            return _
        lax.fori_loop(0, chunks, out, 0)


def place():
    chips = lax.axis_size("dp") // 2
    me = lax.axis_index("dp")
    chip, core = me // 2, lax.rem(me, 2)
    right, left = lax.rem(chip + 1, chips), lax.rem(chip + chips - 1, chips)
    return chips, chip, core, right, left, lax.rem(chip + 2, chips)


def wide_sum(*terms):
    total = terms[0].astype(F32)
    for term in terms[1:]:
        total = total + term.astype(F32)
    return total


class Exchange:
    def __init__(self, tiles, gathered, all_ref, own_ref, g, half, near, far, own, squares, send, recv, local):
        self.tiles, self.gathered, self.all_ref, self.own_ref = tiles, gathered, all_ref, own_ref
        self.g, self.half, self.near, self.far, self.own, self.squares = g, half, near, far, own, squares
        self.send, self.recv, self.local = send, recv, local
        self.chips, self.chip, self.core, self.right, self.left, self.across = place()
        self.depth, self.width = own.shape[1], own.shape[2]
        self.mid = self.width // 2

    def copy(self, kind, t, src, dst, chip=None, core=None):
        to = (self.chip if chip is None else chip) * 2 + (self.core if core is None else core)
        return pltpu.make_async_remote_copy(
            src_ref=src, dst_ref=dst, send_sem=self.send.at[kind, t], recv_sem=self.recv.at[kind, t], device_id={"dp": to}, device_id_type=MESH
        )

    def rows(self, chip, core=None):
        core = self.core if core is None else core
        return pl.ds(pl.multiple_of((core * self.chips + chip) * self.depth, 16), self.depth)

    def within(self, chip):
        return pl.ds(pl.multiple_of(chip * self.depth, 16), self.depth)

    def swap(self, t):
        theirs = pl.ds(pl.multiple_of((1 - self.core) * self.chips * self.depth, 16), self.chips * self.depth)
        return self.copy(0, t, self.g.at[lax.rem(t, SLOTS), theirs, :], self.half.at[lax.rem(t, HALF_SLOTS)], core=1 - self.core)

    def first(self, t):
        slot, r = lax.rem(t, SLOTS), self.rows(self.across)
        return (
            self.copy(1, t, self.g.at[slot, r, pl.ds(0, self.mid)], self.near.at[0, lax.rem(t, RING_SLOTS)], chip=self.right),
            self.copy(2, t, self.g.at[slot, r, pl.ds(self.mid, self.mid)], self.near.at[1, lax.rem(t, RING_SLOTS)], chip=self.left),
        )

    def second(self, t):
        slot = lax.rem(t, SLOTS)
        return (
            self.copy(3, t, self.g.at[slot, self.rows(self.right), :], self.far.at[0, lax.rem(t, RING_SLOTS)], chip=self.right),
            self.copy(4, t, self.g.at[slot, self.rows(self.left), :], self.far.at[1, lax.rem(t, RING_SLOTS)], chip=self.left),
        )

    def cols(self, t, start=0, size=None):
        return pl.ds(pl.multiple_of(t * self.width + start, 128), self.width if size is None else size)

    def region(self, chip, t, start=0, size=None):
        return self.all_ref.at[self.rows(chip), self.cols(t, start, size)]

    def spread(self, t):
        there = self.region(self.chip, t)
        return (
            self.copy(5, t, self.own.at[t], there, chip=self.right),
            self.copy(6, t, self.own.at[t], there, chip=self.left),
            self.copy(7, t, self.own.at[t], there, core=1 - self.core),
        )

    def onward(self, t):
        one, two = self.region(self.left, t, 0, self.mid), self.region(self.right, t, self.mid, self.mid)
        return (self.copy(8, t, one, one, chip=self.right), self.copy(9, t, two, two, chip=self.left))

    def across_chip(self, t):
        one, two = self.region(self.left, t), self.region(self.right, t)
        return (self.copy(10, t, one, one, core=1 - self.core), self.copy(11, t, two, two, core=1 - self.core))

    def last(self, t):
        it = self.region(self.across, t)
        return self.copy(12, t, it, it, core=1 - self.core)

    def kept(self, t):
        return pltpu.make_async_copy(self.own.at[t], self.region(self.chip, t), self.local.at[t])

    def kept_alone(self, t):
        return pltpu.make_async_copy(self.own.at[t], self.own_ref.at[:, self.cols(t - self.gathered)], self.local.at[t])

    def stage(self, j, lag, what, start, stop):
        t = j - lag

        @pl.when((t >= start) & (t < stop))
        def _():
            what(t)

    def step(self, j):
        everyone, alone = (0, self.gathered), (self.gathered, self.tiles)
        self.stage(j, 0, lambda t: self.swap(t).start(), 0, self.tiles)
        self.stage(j, 6, self.finish, *everyone)
        self.stage(j, 5, self.forward_far, *everyone)
        self.stage(j, 4, self.forward_near, *everyone)
        self.stage(j, 4, lambda t: self.kept_alone(t).wait(), *alone)
        self.stage(j, 3, self.own_block, 0, self.tiles)
        self.stage(j, 2, self.neighbours, 0, self.tiles)
        self.stage(j, 1, self.far_block, 0, self.tiles)

    def far_block(self, t):
        self.swap(t).wait_recv()
        slot, r = lax.rem(t, SLOTS), self.rows(self.across)
        self.g[slot, r, :] = wide_sum(self.g[slot, r, :], self.half[lax.rem(t, HALF_SLOTS), self.within(self.across), :]).astype(BF16)
        for one in self.first(t):
            one.start()

    def neighbours(self, t):
        slot, mid = lax.rem(t, SLOTS), self.mid
        for one in self.first(t):
            one.wait_recv()
        for chip, side in ((self.right, 0), (self.left, 1)):
            r, h = self.rows(chip), self.within(chip)
            met, other = pl.ds(side * mid, mid), pl.ds((1 - side) * mid, mid)
            self.g[slot, r, met] = wide_sum(self.g[slot, r, met], self.half[lax.rem(t, HALF_SLOTS), h, met], self.near[side, lax.rem(t, RING_SLOTS)]).astype(BF16)
            self.g[slot, r, other] = wide_sum(self.g[slot, r, other], self.half[lax.rem(t, HALF_SLOTS), h, other]).astype(BF16)
        for one in self.second(t):
            one.start()

    def own_block(self, t):
        slot = lax.rem(t, SLOTS)
        for one in self.second(t):
            one.wait_recv()
        total = wide_sum(self.g[slot, self.rows(self.chip), :], self.half[lax.rem(t, HALF_SLOTS), self.within(self.chip), :], self.far[0, lax.rem(t, RING_SLOTS)], self.far[1, lax.rem(t, RING_SLOTS)]).astype(BF16)
        self.own[t] = total
        wide = total.astype(F32)
        self.squares[...] += jnp.sum((wide * wide).reshape(-1, 8, 128), axis=0)

        @pl.when(t < self.gathered)
        def _():
            self.kept(t).start()
            for one in self.spread(t):
                one.start()

        @pl.when(t >= self.gathered)
        def _():
            self.kept_alone(t).start()

        for one in (self.swap(t), *self.first(t), *self.second(t)):
            one.wait_send()

    def forward_near(self, t):
        right, left, _ = self.spread(t)
        right.wait_recv()
        left.wait_recv()
        for one in (*self.onward(t), *self.across_chip(t)):
            one.start()

    def forward_far(self, t):
        for one in self.onward(t):
            one.wait_recv()
        self.last(t).start()

    def finish(self, t):
        self.kept(t).wait()
        right, left, other = self.spread(t)
        other.wait_recv()
        for one in self.across_chip(t):
            one.wait_recv()
        self.last(t).wait_recv()
        for one in (right, left, other, *self.onward(t), *self.across_chip(t), self.last(t)):
            one.wait_send()


def greet(everyone):
    chips, chip, core, right, left, _ = place()
    barrier = pltpu.get_barrier_semaphore()
    if everyone:
        me = lax.axis_index("dp")
        others = [lax.rem(me + k, 2 * chips) for k in range(1, 2 * chips)]
    else:
        others = [right * 2 + core, left * 2 + core, chip * 2 + 1 - core]
    for other in others:
        pl.semaphore_signal(barrier, inc=1, device_id={"dp": other}, device_id_type=MESH)
    pl.semaphore_wait(barrier, len(others))


def tile_gradients(g, slot, at, dyt, dgate, dup, act):
    g[slot, :, 0:TILE] = nn(at[...], dgate[...]).astype(BF16)
    g[slot, :, TILE : 2 * TILE] = nn(at[...], dup[...]).astype(BF16)
    g[slot, :, 2 * TILE : 3 * TILE] = nn(dyt[...], act[...]).astype(BF16)


def activations(gate, up, d, act, dgate, dup, r):
    s = sigmoid(gate)
    silu = gate * s
    act[r, :] = (silu * up).astype(BF16)
    d_up = (d * silu).astype(BF16)
    d_gate = (d * up * (s + silu * (1.0 - s))).astype(BF16)
    dup[r, :] = d_up
    dgate[r, :] = d_gate
    return d_gate, d_up


def backward_kernel(tiles, left, count, h_ref, dy_ref, at_ref, gate_ref, up_ref, wg_ref, wu_ref, wd_ref, all_ref, own_ref, factor_ref,
                    a, at, dyt, act, dgate, dup, wide, wg, wu, wd, loaded, all_squares, sent, arrived, *comm):
    j = pl.program_id(0)
    d = h_ref.shape[1]
    tokens = h_ref.shape[0]
    exchange = Exchange(2 * tiles, tiles, all_ref, own_ref, *comm)
    at_end = (j == tiles - 1) | (j == 2 * tiles - 1)
    acc = wide.at[:, 0:d]

    def saved(i):
        cols = pl.ds(pl.multiple_of(i * TILE, 128), TILE)
        return (
            pltpu.make_async_copy(gate_ref.at[:, cols], wide.at[:, 0:TILE], loaded.at[0]),
            pltpu.make_async_copy(up_ref.at[:, cols], wide.at[:, TILE : 2 * TILE], loaded.at[1]),
        )

    @pl.when(j == 0)
    def _():
        greet(True)
        exchange.squares[...] = jnp.zeros_like(exchange.squares)

        def norm(c, _):
            r = rows_of(c)
            x = h_ref[r, :].astype(F32)
            normed = (x * scale_of(x)).astype(BF16)
            at[:, r] = normed.T
            dyt[:, r] = dy_ref[r, :].T
            a[r, :] = normed
            acc[r, :] = jnp.zeros((CHUNK, d), F32)
            return _
        lax.fori_loop(0, tokens // CHUNK, norm, 0)

    @pl.when(j < tiles)
    def _():
        hold(wg_ref, wg, 1, left, at_end)
        hold(wu_ref, wu, 1, left, at_end)
        hold(wd_ref, wd, 0, left, at_end)

        def body(c, _):
            r = rows_of(c)
            gate = nn(a[r, :], wg[...])
            up = nn(a[r, :], wu[...])
            d = nt(dy_ref[r, :], wd[...]).astype(BF16).astype(F32)
            d_gate, d_up = activations(gate, up, d, act, dgate, dup, r)
            acc[r, :] += nt(d_gate, wg[...]) + nt(d_up, wu[...])
            return _
        lax.fori_loop(0, tokens // CHUNK, body, 0)

    @pl.when(j == tiles)
    def _():
        normed = pltpu.make_async_copy(at_ref, at, loaded.at[2])
        normed.start()

        def out(c, _):
            r = rows_of(c)
            x = h_ref[r, :].astype(F32)
            scale = scale_of(x)
            da = acc[r, :].astype(BF16).astype(F32)
            dot = jnp.mean(da * x, -1, keepdims=True)
            by = scale * da - x * (scale * scale * scale * dot)
            dh = (dy_ref[r, :].astype(F32) + by.astype(BF16).astype(F32)).astype(BF16)
            a[r, :] = dh
            dyt[:, r] = dh.T
            return _
        lax.fori_loop(0, tokens // CHUNK, out, 0)
        for one in saved(0):
            one.start()
        normed.wait()

    @pl.when((j >= tiles) & (j < 2 * tiles))
    def _():
        hold(wd_ref, wd, 0, left, at_end)
        for one in saved(j - tiles):
            one.wait()
        for c in range(tokens // WIDE):
            r = pl.ds(c * WIDE, WIDE)
            d = nt(a[r, :], wd[...]).astype(BF16).astype(F32)
            activations(wide[r, 0:TILE], wide[r, TILE : 2 * TILE], d, act, dgate, dup, r)

        @pl.when(j < 2 * tiles - 1)
        def _():
            for one in saved(j - tiles + 1):
                one.start()

    @pl.when(j < 2 * tiles)
    def _():
        tile_gradients(exchange.g, lax.rem(j, SLOTS), at, dyt, dgate, dup, act)

    exchange.step(j)

    @pl.when(j == pl.num_programs(0) - 1)
    def _():
        me = lax.axis_index("dp")
        n = lax.axis_size("dp")
        all_squares[me] = exchange.squares[...]
        copies = [
            pltpu.make_async_remote_copy(
                src_ref=exchange.squares, dst_ref=all_squares.at[me], send_sem=sent.at[k], recv_sem=arrived.at[k],
                device_id={"dp": lax.rem(me + k, n)}, device_id_type=MESH,
            )
            for k in range(1, n)
        ]
        for one in copies:
            one.start()
        for one in copies:
            one.wait()
        mean = jnp.sum(all_squares[...]) / count
        factor_ref[...] = jnp.full(factor_ref.shape, jnp.minimum(1.0, 0.5 * lax.rsqrt(mean + 1e-30)), F32)


def whole(shape):
    return pl.BlockSpec(shape, lambda j: (0,) * len(shape), pipeline_mode=pl.Buffered(1))


def params():
    return pltpu.CompilerParams(dimension_semantics=("arbitrary",), vmem_limit_bytes=62 * 1024 * 1024)


def forward(x, w, layer):
    tokens, d = x.shape
    ff = w[0].shape[2]
    tiles = pl.cdiv(ff, TILE)
    col = pl.BlockSpec((1, d, TILE), lambda j: (layer, 0, j))
    row = pl.BlockSpec((1, TILE, d), lambda j: (layer, j, 0))
    saved = pl.BlockSpec((tokens, TILE), lambda j: (0, j))
    return pl.pallas_call(
        functools.partial(forward_kernel, tokens // CHUNK, ff - (tiles - 1) * TILE),
        grid=(tiles,),
        in_specs=[whole((tokens, d)), col, col, row],
        out_specs=[whole((tokens, d)), whole((d, tokens)), saved, saved],
        out_shape=[jax.ShapeDtypeStruct((tokens, d), BF16), jax.ShapeDtypeStruct((d, tokens), BF16)] + [jax.ShapeDtypeStruct((tokens, tiles * TILE), F32)] * 2,
        scratch_shapes=[pltpu.VMEM((tokens, d), BF16), pltpu.VMEM((tokens, d), F32), pltpu.VMEM((d, TILE), BF16), pltpu.VMEM((d, TILE), BF16), pltpu.VMEM((TILE, d), BF16)],
        compiler_params=params(),
        cost_estimate=pl.CostEstimate(flops=6 * tokens * d * ff, bytes_accessed=8 * tokens * ff, transcendentals=tokens * ff),
        name="forward",
    )(x, *w)


def backward(h, dy, at, gate, up, w, n, count):
    tokens, d = h.shape
    ff = w[0].shape[2]
    tiles = pl.cdiv(ff, TILE)
    width, depth = 3 * TILE, d // n

    def late(j):
        return jnp.where(j < tiles, 1, 0)

    def tile(j):
        return jnp.minimum(jnp.where(j < tiles, j, j - tiles), tiles - 1)

    col = pl.BlockSpec((1, d, TILE), lambda j: (1, 0, jnp.minimum(j, tiles - 1)))
    row = pl.BlockSpec((1, TILE, d), lambda j: (late(j), tile(j), 0))
    hbm = pl.BlockSpec(memory_space=pl.ANY)
    return pl.pallas_call(
        functools.partial(backward_kernel, tiles, ff - (tiles - 1) * TILE, count),
        grid=(2 * tiles + 5,),
        in_specs=[whole((tokens, d)), whole((tokens, d)), hbm, hbm, hbm, col, col, row],
        out_specs=[hbm, hbm, whole((8, 128))],
        out_shape=[
            jax.ShapeDtypeStruct((d, width * tiles), BF16),
            jax.ShapeDtypeStruct((depth, width * tiles), BF16),
            jax.ShapeDtypeStruct((8, 128), F32),
        ],
        scratch_shapes=[
            pltpu.VMEM((tokens, d), BF16),
            pltpu.VMEM((d, tokens), BF16),
            pltpu.VMEM((d, tokens), BF16),
            pltpu.VMEM((tokens, TILE), BF16),
            pltpu.VMEM((tokens, TILE), BF16),
            pltpu.VMEM((tokens, TILE), BF16),
            pltpu.VMEM((tokens, 2 * TILE), F32),
            pltpu.VMEM((d, TILE), BF16),
            pltpu.VMEM((d, TILE), BF16),
            pltpu.VMEM((TILE, d), BF16),
            pltpu.SemaphoreType.DMA((3,)),
            pltpu.VMEM((n, 8, 128), F32),
            pltpu.SemaphoreType.DMA((n,)),
            pltpu.SemaphoreType.DMA((n,)),
            pltpu.VMEM((SLOTS, d, width), BF16),
            pltpu.VMEM((HALF_SLOTS, d // 2, width), BF16),
            pltpu.VMEM((2, RING_SLOTS, depth, width // 2), BF16),
            pltpu.VMEM((2, RING_SLOTS, depth, width), BF16),
            pltpu.VMEM((2 * tiles, depth, width), BF16),
            pltpu.VMEM((8, 128), F32),
            pltpu.SemaphoreType.DMA((13, 2 * tiles)),
            pltpu.SemaphoreType.DMA((13, 2 * tiles)),
            pltpu.SemaphoreType.DMA((2 * tiles,)),
        ],
        compiler_params=pltpu.CompilerParams(
            dimension_semantics=("arbitrary",), vmem_limit_bytes=67_000_000, collective_id=0, has_side_effects=True
        ),
        cost_estimate=pl.CostEstimate(flops=24 * tokens * d * ff, bytes_accessed=8 * tokens * ff, transcendentals=2 * tokens * ff),
        name="backward",
    )(h, dy, at, gate, up, *w)


def adamw_kernel(fresh, order, factor_ref, g_ref, *refs):
    w_refs, m_refs, v_refs = refs[0:3], refs[3:6], refs[6:9]
    outs = refs[9:] if fresh else refs[18:]
    factor = factor_ref[0, 0]
    for i in range(3):
        part = g_ref[:, i * TILE : (i + 1) * TILE]
        if order is not None:
            depth = part.shape[0] // len(order)
            part = jnp.concatenate([part[p * depth : (p + 1) * depth] for p in order])
        g = part.astype(F32) * factor
        if i == 2:
            g = g.T
        m = 0.9 * m_refs[i][0] + 0.1 * g
        v = 0.95 * v_refs[i][0] + 0.05 * g * g
        w = w_refs[i][0].astype(F32)
        outs[i][0] = (w - 0.02 * (m * lax.rsqrt(v + 1e-8) + 0.1 * w)).astype(BF16)
        outs[3 + i][0] = m
        outs[6 + i][0] = v


def adamw(factor, g, w, m, v, layer, order=None, so_far=None):
    layers, d, ff = w[0].shape
    tiles = pl.cdiv(ff, TILE)
    col = pl.BlockSpec((1, d, TILE), lambda j: (layer, 0, j))
    row = pl.BlockSpec((1, TILE, d), lambda j: (layer, j, 0))
    nine = [col, col, row] * 3
    arrays = [*w, *m, *v]
    held = [] if so_far is None else list(so_far)
    return pl.pallas_call(
        functools.partial(adamw_kernel, so_far is None, order),
        grid=(tiles,),
        in_specs=[pl.BlockSpec(memory_space=pltpu.SMEM), pl.BlockSpec((d, 3 * TILE), lambda j: (0, j))] + nine + [pl.BlockSpec(memory_space=pl.ANY)] * len(held),
        out_specs=nine,
        out_shape=[jax.ShapeDtypeStruct(a.shape, a.dtype) for a in arrays],
        input_output_aliases={11 + i: i for i in range(len(held))},
        compiler_params=params(),
        cost_estimate=pl.CostEstimate(flops=60 * d * ff, bytes_accessed=66 * d * ff, transcendentals=3 * d * ff),
        name="adamw",
    )(factor, g, *arrays, *held)


def solution(mesh):
    n = mesh.shape["dp"]
    order = [chip * 2 + core for core in range(2) for chip in range(n // 2)]

    def step(x, dy, *arrays):
        w, m, v = (arrays[i : i + 3] for i in (0, 3, 6))
        x, dy = x[0], dy[0]
        h, at, gate, up = forward(x, w, 0)
        g1, s0, factor = backward(h, dy, at, gate, up, w, n, sum(a.size for a in w))
        g0 = lax.all_gather(s0, "dp", axis=0, tiled=True)
        new = adamw(factor, g1, w, m, v, 1)
        return tuple(adamw(factor, g0, w, m, v, 0, order, new))

    return jax.shard_map(
        step,
        mesh=mesh,
        in_specs=(P(("rep", "dp"), None, None),) * 2 + (P(None, None, None),) * 9,
        out_specs=(P("rep", None, None),) * 9,
        check_vma=False,
    )
```

```python
import functools
import jax
import jax.numpy as jnp
from jax import lax
from jax.experimental import pallas as pl
from jax.experimental.pallas import tpu as pltpu
from jax.sharding import PartitionSpec as P

F32, BF16 = jnp.float32, jnp.bfloat16
TILE = 512
CHUNK = 1024
WIDE = 2048
SLOTS, HALF_SLOTS, RING_SLOTS = 4, 6, 4
MESH = pl.DeviceIdType.MESH


def nn(a, b):
    return jnp.dot(a, b, preferred_element_type=F32)


def nt(a, b):
    return lax.dot_general(a, b, (((1,), (1,)), ((), ())), preferred_element_type=F32)


def scale_of(wide):
    return lax.rsqrt(jnp.mean(wide * wide, -1, keepdims=True) + 1e-6)


def sigmoid(x):
    return 0.5 * jnp.tanh(0.5 * x) + 0.5


def rows_of(c):
    return pl.ds(pl.multiple_of(c * CHUNK, CHUNK), CHUNK)


def hold(ref, kept, axis, left, at_end):
    kept[...] = ref[0]
    if left < TILE:
        @pl.when(at_end)
        def _():
            if axis == 1:
                kept[:, left:] = jnp.zeros((kept.shape[0], TILE - left), kept.dtype)
            else:
                kept[left:, :] = jnp.zeros((TILE - left, kept.shape[1]), kept.dtype)


def forward_kernel(chunks, left, x_ref, wg_ref, wu_ref, wd_ref, h_ref, at_ref, gate_ref, up_ref, a, acc, wg, wu, wd):
    j = pl.program_id(0)

    @pl.when(j == 0)
    def _():
        def norm(c, _):
            wide = x_ref[rows_of(c), :].astype(F32)
            normed = (wide * scale_of(wide)).astype(BF16)
            a[rows_of(c), :] = normed
            at_ref[:, rows_of(c)] = normed.T
            acc[rows_of(c), :] = jnp.zeros((CHUNK, acc.shape[1]), F32)
            return _
        lax.fori_loop(0, chunks, norm, 0)

    hold(wg_ref, wg, 1, left, j == pl.num_programs(0) - 1)
    hold(wu_ref, wu, 1, left, j == pl.num_programs(0) - 1)
    hold(wd_ref, wd, 0, left, j == pl.num_programs(0) - 1)

    def body(c, _):
        r = rows_of(c)
        gate = nn(a[r, :], wg[...])
        up = nn(a[r, :], wu[...])
        gate_ref[r, :] = gate
        up_ref[r, :] = up
        act = (gate * sigmoid(gate) * up).astype(BF16)
        acc[r, :] += nn(act, wd[...])
        return _
    lax.fori_loop(0, chunks, body, 0)

    @pl.when(j == pl.num_programs(0) - 1)
    def _():
        def out(c, _):
            r = rows_of(c)
            h_ref[r, :] = (x_ref[r, :].astype(F32) + acc[r, :].astype(BF16).astype(F32)).astype(BF16)
            return _
        lax.fori_loop(0, chunks, out, 0)


def place():
    chips = lax.axis_size("dp") // 2
    me = lax.axis_index("dp")
    chip, core = me // 2, lax.rem(me, 2)
    right, left = lax.rem(chip + 1, chips), lax.rem(chip + chips - 1, chips)
    return chips, chip, core, right, left, lax.rem(chip + 2, chips)


def wide_sum(*terms):
    total = terms[0].astype(F32)
    for term in terms[1:]:
        total = total + term.astype(F32)
    return total


class Exchange:
    def __init__(self, tiles, gathered, all_ref, own_ref, g, half, near, far, own, squares, send, recv, local):
        self.tiles, self.gathered, self.all_ref, self.own_ref = tiles, gathered, all_ref, own_ref
        self.g, self.half, self.near, self.far, self.own, self.squares = g, half, near, far, own, squares
        self.send, self.recv, self.local = send, recv, local
        self.chips, self.chip, self.core, self.right, self.left, self.across = place()
        self.depth, self.width = own.shape[1], own.shape[2]
        self.mid = self.width // 2

    def copy(self, kind, t, src, dst, chip=None, core=None):
        to = (self.chip if chip is None else chip) * 2 + (self.core if core is None else core)
        return pltpu.make_async_remote_copy(
            src_ref=src, dst_ref=dst, send_sem=self.send.at[kind, t], recv_sem=self.recv.at[kind, t], device_id={"dp": to}, device_id_type=MESH
        )

    def rows(self, chip, core=None):
        core = self.core if core is None else core
        return pl.ds(pl.multiple_of((core * self.chips + chip) * self.depth, 16), self.depth)

    def within(self, chip):
        return pl.ds(pl.multiple_of(chip * self.depth, 16), self.depth)

    def swap(self, t):
        theirs = pl.ds(pl.multiple_of((1 - self.core) * self.chips * self.depth, 16), self.chips * self.depth)
        return self.copy(0, t, self.g.at[lax.rem(t, SLOTS), theirs, :], self.half.at[lax.rem(t, HALF_SLOTS)], core=1 - self.core)

    def first(self, t):
        slot, r = lax.rem(t, SLOTS), self.rows(self.across)
        return (
            self.copy(1, t, self.g.at[slot, r, pl.ds(0, self.mid)], self.near.at[0, lax.rem(t, RING_SLOTS)], chip=self.right),
            self.copy(2, t, self.g.at[slot, r, pl.ds(self.mid, self.mid)], self.near.at[1, lax.rem(t, RING_SLOTS)], chip=self.left),
        )

    def second(self, t):
        slot = lax.rem(t, SLOTS)
        return (
            self.copy(3, t, self.g.at[slot, self.rows(self.right), :], self.far.at[0, lax.rem(t, RING_SLOTS)], chip=self.right),
            self.copy(4, t, self.g.at[slot, self.rows(self.left), :], self.far.at[1, lax.rem(t, RING_SLOTS)], chip=self.left),
        )

    def cols(self, t, start=0, size=None):
        return pl.ds(pl.multiple_of(t * self.width + start, 128), self.width if size is None else size)

    def region(self, chip, t, start=0, size=None):
        return self.all_ref.at[self.rows(chip), self.cols(t, start, size)]

    def spread(self, t):
        there = self.region(self.chip, t)
        return (
            self.copy(5, t, self.own.at[t], there, chip=self.right),
            self.copy(6, t, self.own.at[t], there, chip=self.left),
            self.copy(7, t, self.own.at[t], there, core=1 - self.core),
        )

    def onward(self, t):
        one, two = self.region(self.left, t, 0, self.mid), self.region(self.right, t, self.mid, self.mid)
        return (self.copy(8, t, one, one, chip=self.right), self.copy(9, t, two, two, chip=self.left))

    def across_chip(self, t):
        one, two = self.region(self.left, t), self.region(self.right, t)
        return (self.copy(10, t, one, one, core=1 - self.core), self.copy(11, t, two, two, core=1 - self.core))

    def last(self, t):
        it = self.region(self.across, t)
        return self.copy(12, t, it, it, core=1 - self.core)

    def kept(self, t):
        return pltpu.make_async_copy(self.own.at[t], self.region(self.chip, t), self.local.at[t])

    def kept_alone(self, t):
        return pltpu.make_async_copy(self.own.at[t], self.own_ref.at[:, self.cols(t - self.gathered)], self.local.at[t])

    def stage(self, j, lag, what, start, stop):
        t = j - lag

        @pl.when((t >= start) & (t < stop))
        def _():
            what(t)

    def early(self, j):
        soon = self.gathered - 1
        self.stage(j, 1, self.far_block, 0, self.tiles)
        self.stage(j, 2, self.neighbours, soon, self.tiles)
        self.stage(j, 2, self.own_block, 0, soon)
        self.stage(j, 3, self.forward_far, 0, soon - 1)

    def midway(self, j):
        self.stage(j, 1, self.neighbours, 0, self.gathered - 1)

    def late(self, j):
        soon = self.gathered - 1
        self.stage(j, 0, lambda t: self.swap(t).start(), 0, self.tiles)
        self.stage(j, 3, self.own_block, soon, self.tiles)
        self.stage(j, 4, lambda t: self.kept_alone(t).wait(), self.gathered, self.tiles)
        self.stage(j, 3, self.finish, 0, soon - 1)
        self.stage(j, 2, self.forward_near, 0, soon - 1)
        for t, lag in ((soon - 1, 3), (soon, 4)):
            self.stage(j, lag, self.forward_near, t, t + 1)
            self.stage(j, lag + 1, self.forward_far, t, t + 1)
            self.stage(j, lag + 2, self.finish, t, t + 1)

    def far_block(self, t):
        self.swap(t).wait_recv()
        slot, r = lax.rem(t, SLOTS), self.rows(self.across)
        self.g[slot, r, :] = wide_sum(self.g[slot, r, :], self.half[lax.rem(t, HALF_SLOTS), self.within(self.across), :]).astype(BF16)
        for one in self.first(t):
            one.start()

    def neighbours(self, t):
        slot, mid = lax.rem(t, SLOTS), self.mid
        for one in self.first(t):
            one.wait_recv()
        for chip, side in ((self.right, 0), (self.left, 1)):
            r, h = self.rows(chip), self.within(chip)
            met, other = pl.ds(side * mid, mid), pl.ds((1 - side) * mid, mid)
            self.g[slot, r, met] = wide_sum(self.g[slot, r, met], self.half[lax.rem(t, HALF_SLOTS), h, met], self.near[side, lax.rem(t, RING_SLOTS)]).astype(BF16)
            self.g[slot, r, other] = wide_sum(self.g[slot, r, other], self.half[lax.rem(t, HALF_SLOTS), h, other]).astype(BF16)
        for one in self.second(t):
            one.start()

    def own_block(self, t):
        slot = lax.rem(t, SLOTS)
        for one in self.second(t):
            one.wait_recv()
        total = wide_sum(self.g[slot, self.rows(self.chip), :], self.half[lax.rem(t, HALF_SLOTS), self.within(self.chip), :], self.far[0, lax.rem(t, RING_SLOTS)], self.far[1, lax.rem(t, RING_SLOTS)]).astype(BF16)
        self.own[t] = total
        wide = total.astype(F32)
        self.squares[...] += jnp.sum((wide * wide).reshape(-1, 8, 128), axis=0)

        @pl.when(t < self.gathered)
        def _():
            self.kept(t).start()
            for one in self.spread(t):
                one.start()

        @pl.when(t >= self.gathered)
        def _():
            self.kept_alone(t).start()

        for one in (self.swap(t), *self.first(t), *self.second(t)):
            one.wait_send()

    def forward_near(self, t):
        right, left, _ = self.spread(t)
        right.wait_recv()
        left.wait_recv()
        for one in (*self.onward(t), *self.across_chip(t)):
            one.start()

    def forward_far(self, t):
        for one in self.onward(t):
            one.wait_recv()
        self.last(t).start()

    def finish(self, t):
        self.kept(t).wait()
        right, left, other = self.spread(t)
        other.wait_recv()
        for one in self.across_chip(t):
            one.wait_recv()
        self.last(t).wait_recv()
        for one in (right, left, other, *self.onward(t), *self.across_chip(t), self.last(t)):
            one.wait_send()


def greet(everyone):
    chips, chip, core, right, left, _ = place()
    barrier = pltpu.get_barrier_semaphore()
    if everyone:
        me = lax.axis_index("dp")
        others = [lax.rem(me + k, 2 * chips) for k in range(1, 2 * chips)]
    else:
        others = [right * 2 + core, left * 2 + core, chip * 2 + 1 - core]
    for other in others:
        pl.semaphore_signal(barrier, inc=1, device_id={"dp": other}, device_id_type=MESH)
    pl.semaphore_wait(barrier, len(others))


def tile_gradients(g, slot, at, dyt, dgate, dup, act):
    g[slot, :, 0:TILE] = nn(at[...], dgate[...]).astype(BF16)
    g[slot, :, TILE : 2 * TILE] = nn(at[...], dup[...]).astype(BF16)
    g[slot, :, 2 * TILE : 3 * TILE] = nn(dyt[...], act[...]).astype(BF16)


def activations(gate, up, d, act, dgate, dup, r):
    s = sigmoid(gate)
    silu = gate * s
    act[r, :] = (silu * up).astype(BF16)
    d_up = (d * silu).astype(BF16)
    d_gate = (d * up * (s + silu * (1.0 - s))).astype(BF16)
    dup[r, :] = d_up
    dgate[r, :] = d_gate
    return d_gate, d_up


def backward_kernel(tiles, left, count, h_ref, dy_ref, at_ref, gate_ref, up_ref, wg_ref, wu_ref, wd_ref, all_ref, own_ref, factor_ref,
                    a, at, dyt, act, dgate, dup, wide, wg, wu, wd, loaded, all_squares, sent, arrived, *comm):
    j = pl.program_id(0)
    d = h_ref.shape[1]
    tokens = h_ref.shape[0]
    exchange = Exchange(2 * tiles, tiles, all_ref, own_ref, *comm)
    at_end = (j == tiles - 1) | (j == 2 * tiles - 1)
    acc = wide.at[:, 0:d]

    def saved(i):
        cols = pl.ds(pl.multiple_of(i * TILE, 128), TILE)
        return (
            pltpu.make_async_copy(gate_ref.at[:, cols], wide.at[:, 0:TILE], loaded.at[0]),
            pltpu.make_async_copy(up_ref.at[:, cols], wide.at[:, TILE : 2 * TILE], loaded.at[1]),
        )

    @pl.when(j == 0)
    def _():
        greet(True)
        exchange.squares[...] = jnp.zeros_like(exchange.squares)

        def norm(c, _):
            r = rows_of(c)
            x = h_ref[r, :].astype(F32)
            normed = (x * scale_of(x)).astype(BF16)
            at[:, r] = normed.T
            dyt[:, r] = dy_ref[r, :].T
            a[r, :] = normed
            acc[r, :] = jnp.zeros((CHUNK, d), F32)
            return _
        lax.fori_loop(0, tokens // CHUNK, norm, 0)

    @pl.when(j < tiles)
    def _():
        hold(wg_ref, wg, 1, left, at_end)
        hold(wu_ref, wu, 1, left, at_end)
        hold(wd_ref, wd, 0, left, at_end)

        def body(c, _):
            r = rows_of(c)
            gate = nn(a[r, :], wg[...])
            up = nn(a[r, :], wu[...])
            d = nt(dy_ref[r, :], wd[...]).astype(BF16).astype(F32)
            d_gate, d_up = activations(gate, up, d, act, dgate, dup, r)
            acc[r, :] += nt(d_gate, wg[...]) + nt(d_up, wu[...])

            @pl.when(c == 0)
            def _():
                exchange.early(j)

            @pl.when(c == 1)
            def _():
                exchange.midway(j)

            return 0
        lax.fori_loop(0, tokens // CHUNK, body, 0)

    @pl.when(j == tiles)
    def _():
        normed = pltpu.make_async_copy(at_ref, at, loaded.at[2])
        normed.start()

        def out(c, _):
            r = rows_of(c)
            x = h_ref[r, :].astype(F32)
            scale = scale_of(x)
            da = acc[r, :].astype(BF16).astype(F32)
            dot = jnp.mean(da * x, -1, keepdims=True)
            by = scale * da - x * (scale * scale * scale * dot)
            dh = (dy_ref[r, :].astype(F32) + by.astype(BF16).astype(F32)).astype(BF16)
            a[r, :] = dh
            dyt[:, r] = dh.T
            return _
        lax.fori_loop(0, tokens // CHUNK, out, 0)
        for one in saved(0):
            one.start()
        normed.wait()

    @pl.when((j >= tiles) & (j < 2 * tiles))
    def _():
        hold(wd_ref, wd, 0, left, at_end)
        for one in saved(j - tiles):
            one.wait()
        for c in range(tokens // WIDE):
            r = pl.ds(c * WIDE, WIDE)
            d = nt(a[r, :], wd[...]).astype(BF16).astype(F32)
            activations(wide[r, 0:TILE], wide[r, TILE : 2 * TILE], d, act, dgate, dup, r)

        @pl.when(j < 2 * tiles - 1)
        def _():
            for one in saved(j - tiles + 1):
                one.start()

    @pl.when(j >= tiles)
    def _():
        exchange.early(j)

    @pl.when(j < 2 * tiles)
    def _():
        tile_gradients(exchange.g, lax.rem(j, SLOTS), at, dyt, dgate, dup, act)

    exchange.late(j)

    @pl.when(j == pl.num_programs(0) - 1)
    def _():
        me = lax.axis_index("dp")
        n = lax.axis_size("dp")
        all_squares[me] = exchange.squares[...]
        copies = [
            pltpu.make_async_remote_copy(
                src_ref=exchange.squares, dst_ref=all_squares.at[me], send_sem=sent.at[k], recv_sem=arrived.at[k],
                device_id={"dp": lax.rem(me + k, n)}, device_id_type=MESH,
            )
            for k in range(1, n)
        ]
        for one in copies:
            one.start()
        for one in copies:
            one.wait()
        mean = jnp.sum(all_squares[...]) / count
        factor_ref[...] = jnp.full(factor_ref.shape, jnp.minimum(1.0, 0.5 * lax.rsqrt(mean + 1e-30)), F32)


def whole(shape):
    return pl.BlockSpec(shape, lambda j: (0,) * len(shape), pipeline_mode=pl.Buffered(1))


def params():
    return pltpu.CompilerParams(dimension_semantics=("arbitrary",), vmem_limit_bytes=62 * 1024 * 1024)


def forward(x, w, layer):
    tokens, d = x.shape
    ff = w[0].shape[2]
    tiles = pl.cdiv(ff, TILE)
    col = pl.BlockSpec((1, d, TILE), lambda j: (layer, 0, j))
    row = pl.BlockSpec((1, TILE, d), lambda j: (layer, j, 0))
    saved = pl.BlockSpec((tokens, TILE), lambda j: (0, j))
    return pl.pallas_call(
        functools.partial(forward_kernel, tokens // CHUNK, ff - (tiles - 1) * TILE),
        grid=(tiles,),
        in_specs=[whole((tokens, d)), col, col, row],
        out_specs=[whole((tokens, d)), whole((d, tokens)), saved, saved],
        out_shape=[jax.ShapeDtypeStruct((tokens, d), BF16), jax.ShapeDtypeStruct((d, tokens), BF16)] + [jax.ShapeDtypeStruct((tokens, tiles * TILE), F32)] * 2,
        scratch_shapes=[pltpu.VMEM((tokens, d), BF16), pltpu.VMEM((tokens, d), F32), pltpu.VMEM((d, TILE), BF16), pltpu.VMEM((d, TILE), BF16), pltpu.VMEM((TILE, d), BF16)],
        compiler_params=params(),
        cost_estimate=pl.CostEstimate(flops=6 * tokens * d * ff, bytes_accessed=8 * tokens * ff, transcendentals=tokens * ff),
        name="forward",
    )(x, *w)


def backward(h, dy, at, gate, up, w, n, count):
    tokens, d = h.shape
    ff = w[0].shape[2]
    tiles = pl.cdiv(ff, TILE)
    width, depth = 3 * TILE, d // n

    def late(j):
        return jnp.where(j < tiles, 1, 0)

    def tile(j):
        return jnp.minimum(jnp.where(j < tiles, j, j - tiles), tiles - 1)

    col = pl.BlockSpec((1, d, TILE), lambda j: (1, 0, jnp.minimum(j, tiles - 1)))
    row = pl.BlockSpec((1, TILE, d), lambda j: (late(j), tile(j), 0))
    hbm = pl.BlockSpec(memory_space=pl.ANY)
    return pl.pallas_call(
        functools.partial(backward_kernel, tiles, ff - (tiles - 1) * TILE, count),
        grid=(2 * tiles + 4,),
        in_specs=[whole((tokens, d)), whole((tokens, d)), hbm, hbm, hbm, col, col, row],
        out_specs=[hbm, hbm, whole((8, 128))],
        out_shape=[
            jax.ShapeDtypeStruct((d, width * tiles), BF16),
            jax.ShapeDtypeStruct((depth, width * tiles), BF16),
            jax.ShapeDtypeStruct((8, 128), F32),
        ],
        scratch_shapes=[
            pltpu.VMEM((tokens, d), BF16),
            pltpu.VMEM((d, tokens), BF16),
            pltpu.VMEM((d, tokens), BF16),
            pltpu.VMEM((tokens, TILE), BF16),
            pltpu.VMEM((tokens, TILE), BF16),
            pltpu.VMEM((tokens, TILE), BF16),
            pltpu.VMEM((tokens, 2 * TILE), F32),
            pltpu.VMEM((d, TILE), BF16),
            pltpu.VMEM((d, TILE), BF16),
            pltpu.VMEM((TILE, d), BF16),
            pltpu.SemaphoreType.DMA((3,)),
            pltpu.VMEM((n, 8, 128), F32),
            pltpu.SemaphoreType.DMA((n,)),
            pltpu.SemaphoreType.DMA((n,)),
            pltpu.VMEM((SLOTS, d, width), BF16),
            pltpu.VMEM((HALF_SLOTS, d // 2, width), BF16),
            pltpu.VMEM((2, RING_SLOTS, depth, width // 2), BF16),
            pltpu.VMEM((2, RING_SLOTS, depth, width), BF16),
            pltpu.VMEM((2 * tiles, depth, width), BF16),
            pltpu.VMEM((8, 128), F32),
            pltpu.SemaphoreType.DMA((13, 2 * tiles)),
            pltpu.SemaphoreType.DMA((13, 2 * tiles)),
            pltpu.SemaphoreType.DMA((2 * tiles,)),
        ],
        compiler_params=pltpu.CompilerParams(
            dimension_semantics=("arbitrary",), vmem_limit_bytes=67_000_000, collective_id=0, has_side_effects=True
        ),
        cost_estimate=pl.CostEstimate(flops=24 * tokens * d * ff, bytes_accessed=8 * tokens * ff, transcendentals=2 * tokens * ff),
        name="backward",
    )(h, dy, at, gate, up, *w)


def adamw_kernel(fresh, order, factor_ref, g_ref, *refs):
    w_refs, m_refs, v_refs = refs[0:3], refs[3:6], refs[6:9]
    outs = refs[9:] if fresh else refs[18:]
    factor = factor_ref[0, 0]
    for i in range(3):
        part = g_ref[:, i * TILE : (i + 1) * TILE]
        if order is not None:
            depth = part.shape[0] // len(order)
            part = jnp.concatenate([part[p * depth : (p + 1) * depth] for p in order])
        g = part.astype(F32) * factor
        if i == 2:
            g = g.T
        m = 0.9 * m_refs[i][0] + 0.1 * g
        v = 0.95 * v_refs[i][0] + 0.05 * g * g
        w = w_refs[i][0].astype(F32)
        outs[i][0] = (w - 0.02 * (m * lax.rsqrt(v + 1e-8) + 0.1 * w)).astype(BF16)
        outs[3 + i][0] = m
        outs[6 + i][0] = v


def adamw(factor, g, w, m, v, layer, order=None, so_far=None):
    layers, d, ff = w[0].shape
    tiles = pl.cdiv(ff, TILE)
    col = pl.BlockSpec((1, d, TILE), lambda j: (layer, 0, j))
    row = pl.BlockSpec((1, TILE, d), lambda j: (layer, j, 0))
    nine = [col, col, row] * 3
    arrays = [*w, *m, *v]
    held = [] if so_far is None else list(so_far)
    return pl.pallas_call(
        functools.partial(adamw_kernel, so_far is None, order),
        grid=(tiles,),
        in_specs=[pl.BlockSpec(memory_space=pltpu.SMEM), pl.BlockSpec((d, 3 * TILE), lambda j: (0, j))] + nine + [pl.BlockSpec(memory_space=pl.ANY)] * len(held),
        out_specs=nine,
        out_shape=[jax.ShapeDtypeStruct(a.shape, a.dtype) for a in arrays],
        input_output_aliases={11 + i: i for i in range(len(held))},
        compiler_params=params(),
        cost_estimate=pl.CostEstimate(flops=60 * d * ff, bytes_accessed=66 * d * ff, transcendentals=3 * d * ff),
        name="adamw",
    )(factor, g, *arrays, *held)


def solution(mesh):
    n = mesh.shape["dp"]
    order = [chip * 2 + core for core in range(2) for chip in range(n // 2)]

    def step(x, dy, *arrays):
        w, m, v = (arrays[i : i + 3] for i in (0, 3, 6))
        x, dy = x[0], dy[0]
        h, at, gate, up = forward(x, w, 0)
        g1, s0, factor = backward(h, dy, at, gate, up, w, n, sum(a.size for a in w))
        g0 = lax.all_gather(s0, "dp", axis=0, tiled=True)
        new = adamw(factor, g1, w, m, v, 1)
        return tuple(adamw(factor, g0, w, m, v, 0, order, new))

    return jax.shard_map(
        step,
        mesh=mesh,
        in_specs=(P(("rep", "dp"), None, None),) * 2 + (P(None, None, None),) * 9,
        out_specs=(P("rep", None, None),) * 9,
        check_vma=False,
    )
```

```python
import functools
import jax
import jax.numpy as jnp
from jax import lax
from jax.experimental import pallas as pl
from jax.experimental.pallas import tpu as pltpu
from jax.sharding import PartitionSpec as P

F32, BF16 = jnp.float32, jnp.bfloat16
TILE = 512
CHUNK = 1024
WIDE = 2048
SLOTS, HALF_SLOTS, RING_SLOTS = 4, 6, 4
ROWS = 8
MESH = pl.DeviceIdType.MESH


def nn(a, b):
    return jnp.dot(a, b, preferred_element_type=F32)


def nt(a, b):
    return lax.dot_general(a, b, (((1,), (1,)), ((), ())), preferred_element_type=F32)


def scale_of(wide):
    return lax.rsqrt(jnp.mean(wide * wide, -1, keepdims=True) + 1e-6)


def sigmoid(x):
    return 0.5 * jnp.tanh(0.5 * x) + 0.5


def rows_of(c):
    return pl.ds(pl.multiple_of(c * CHUNK, CHUNK), CHUNK)


def hold(ref, kept, axis, left, at_end):
    kept[...] = ref[0]
    if left < TILE:
        @pl.when(at_end)
        def _():
            if axis == 1:
                kept[:, left:] = jnp.zeros((kept.shape[0], TILE - left), kept.dtype)
            else:
                kept[left:, :] = jnp.zeros((TILE - left, kept.shape[1]), kept.dtype)


def forward_kernel(chunks, left, x_ref, wg_ref, wu_ref, wd_ref, h_ref, at_ref, gate_ref, up_ref, a, acc, wg, wu, wd):
    j = pl.program_id(0)

    @pl.when(j == 0)
    def _():
        def norm(c, _):
            wide = x_ref[rows_of(c), :].astype(F32)
            normed = (wide * scale_of(wide)).astype(BF16)
            a[rows_of(c), :] = normed
            at_ref[:, rows_of(c)] = normed.T
            acc[rows_of(c), :] = jnp.zeros((CHUNK, acc.shape[1]), F32)
            return _
        lax.fori_loop(0, chunks, norm, 0)

    hold(wg_ref, wg, 1, left, j == pl.num_programs(0) - 1)
    hold(wu_ref, wu, 1, left, j == pl.num_programs(0) - 1)
    hold(wd_ref, wd, 0, left, j == pl.num_programs(0) - 1)

    def body(c, _):
        r = rows_of(c)
        gate = nn(a[r, :], wg[...])
        up = nn(a[r, :], wu[...])
        gate_ref[r, :] = gate
        up_ref[r, :] = up
        act = (gate * sigmoid(gate) * up).astype(BF16)
        acc[r, :] += nn(act, wd[...])
        return _
    lax.fori_loop(0, chunks, body, 0)

    @pl.when(j == pl.num_programs(0) - 1)
    def _():
        def out(c, _):
            r = rows_of(c)
            h_ref[r, :] = (x_ref[r, :].astype(F32) + acc[r, :].astype(BF16).astype(F32)).astype(BF16)
            return _
        lax.fori_loop(0, chunks, out, 0)


def place():
    chips = lax.axis_size("dp") // 2
    me = lax.axis_index("dp")
    chip, core = me // 2, lax.rem(me, 2)
    right, left = lax.rem(chip + 1, chips), lax.rem(chip + chips - 1, chips)
    return chips, chip, core, right, left, lax.rem(chip + 2, chips)


def wide_sum(*terms):
    total = terms[0].astype(F32)
    for term in terms[1:]:
        total = total + term.astype(F32)
    return total


class Exchange:
    def __init__(self, tiles, gathered, all_ref, own_ref, g, half, near, far, own, squares, send, recv, local):
        self.tiles, self.gathered, self.all_ref, self.own_ref = tiles, gathered, all_ref, own_ref
        self.g, self.half, self.near, self.far, self.own, self.squares = g, half, near, far, own, squares
        self.send, self.recv, self.local = send, recv, local
        self.chips, self.chip, self.core, self.right, self.left, self.across = place()
        self.depth, self.width = own.shape[1], own.shape[2]
        self.mid = self.width // 2
        self.split = gathered + own_ref[0].shape[1] // self.width

    def copy(self, kind, t, src, dst, chip=None, core=None):
        to = (self.chip if chip is None else chip) * 2 + (self.core if core is None else core)
        return pltpu.make_async_remote_copy(
            src_ref=src, dst_ref=dst, send_sem=self.send.at[kind, t], recv_sem=self.recv.at[kind, t], device_id={"dp": to}, device_id_type=MESH
        )

    def rows(self, chip, core=None):
        core = self.core if core is None else core
        return pl.ds(pl.multiple_of((core * self.chips + chip) * self.depth, 16), self.depth)

    def within(self, chip):
        return pl.ds(pl.multiple_of(chip * self.depth, 16), self.depth)

    def swap(self, t):
        theirs = pl.ds(pl.multiple_of((1 - self.core) * self.chips * self.depth, 16), self.chips * self.depth)
        return self.copy(0, t, self.g.at[lax.rem(t, SLOTS), theirs, :], self.half.at[lax.rem(t, HALF_SLOTS)], core=1 - self.core)

    def first(self, t):
        slot, r = lax.rem(t, SLOTS), self.rows(self.across)
        return (
            self.copy(1, t, self.g.at[slot, r, pl.ds(0, self.mid)], self.near.at[0, lax.rem(t, RING_SLOTS)], chip=self.right),
            self.copy(2, t, self.g.at[slot, r, pl.ds(self.mid, self.mid)], self.near.at[1, lax.rem(t, RING_SLOTS)], chip=self.left),
        )

    def second(self, t):
        slot = lax.rem(t, SLOTS)
        return (
            self.copy(3, t, self.g.at[slot, self.rows(self.right), :], self.far.at[0, lax.rem(t, RING_SLOTS)], chip=self.right),
            self.copy(4, t, self.g.at[slot, self.rows(self.left), :], self.far.at[1, lax.rem(t, RING_SLOTS)], chip=self.left),
        )

    def cols(self, t, start=0, size=None):
        return pl.ds(pl.multiple_of(t * self.width + start, 128), self.width if size is None else size)

    def region(self, chip, t, start=0, size=None):
        return self.all_ref.at[self.rows(chip), self.cols(t, start, size)]

    def spread(self, t):
        there = self.region(self.chip, t)
        return (
            self.copy(5, t, self.own.at[t], there, chip=self.right),
            self.copy(6, t, self.own.at[t], there, chip=self.left),
            self.copy(7, t, self.own.at[t], there, core=1 - self.core),
        )

    def onward(self, t):
        one, two = self.region(self.left, t, 0, self.mid), self.region(self.right, t, self.mid, self.mid)
        return (self.copy(8, t, one, one, chip=self.right), self.copy(9, t, two, two, chip=self.left))

    def across_chip(self, t):
        one, two = self.region(self.left, t), self.region(self.right, t)
        return (self.copy(10, t, one, one, core=1 - self.core), self.copy(11, t, two, two, core=1 - self.core))

    def last(self, t):
        it = self.region(self.across, t)
        return self.copy(12, t, it, it, core=1 - self.core)

    def kept(self, t):
        return pltpu.make_async_copy(self.own.at[t], self.region(self.chip, t), self.local.at[t])

    def kept_alone(self, t, part):
        ref = self.own_ref[part]
        start = self.gathered if part == 0 else self.split
        return pltpu.make_async_copy(self.own.at[t], ref.at[:, self.cols(t - start)], self.local.at[t])

    def stage(self, j, lag, what, start, stop):
        t = j - lag

        @pl.when((t >= start) & (t < stop))
        def _():
            what(t)

    def early(self, j):
        soon = self.gathered - 1
        self.stage(j, 1, self.far_block, 0, self.tiles)
        self.stage(j, 2, self.neighbours, soon, self.tiles)
        self.stage(j, 2, self.own_block, 0, soon)
        self.stage(j, 3, self.forward_far, 0, soon - 1)

    def midway(self, j):
        self.stage(j, 1, self.neighbours, 0, self.gathered - 1)

    def late(self, j):
        soon = self.gathered - 1
        self.stage(j, 0, lambda t: self.swap(t).start(), 0, self.tiles)
        self.stage(j, 3, self.own_block, soon, self.tiles)
        self.stage(j, 4, lambda t: self.kept_alone(t, 0).wait(), self.gathered, self.split)
        self.stage(j, 4, lambda t: self.kept_alone(t, 1).wait(), self.split, self.tiles)
        self.stage(j, 3, self.finish, 0, soon - 1)
        self.stage(j, 2, self.forward_near, 0, soon - 1)
        for t, lag in ((soon - 1, 3), (soon, 4)):
            self.stage(j, lag, self.forward_near, t, t + 1)
            self.stage(j, lag + 1, self.forward_far, t, t + 1)
            self.stage(j, lag + 2, self.finish, t, t + 1)

    def far_block(self, t):
        self.swap(t).wait_recv()
        slot, r = lax.rem(t, SLOTS), self.rows(self.across)
        self.g[slot, r, :] = wide_sum(self.g[slot, r, :], self.half[lax.rem(t, HALF_SLOTS), self.within(self.across), :]).astype(BF16)
        for one in self.first(t):
            one.start()

    def neighbours(self, t):
        slot, mid = lax.rem(t, SLOTS), self.mid
        for one in self.first(t):
            one.wait_recv()
        for chip, side in ((self.right, 0), (self.left, 1)):
            r, h = self.rows(chip), self.within(chip)
            met, other = pl.ds(side * mid, mid), pl.ds((1 - side) * mid, mid)
            self.g[slot, r, met] = wide_sum(self.g[slot, r, met], self.half[lax.rem(t, HALF_SLOTS), h, met], self.near[side, lax.rem(t, RING_SLOTS)]).astype(BF16)
            self.g[slot, r, other] = wide_sum(self.g[slot, r, other], self.half[lax.rem(t, HALF_SLOTS), h, other]).astype(BF16)
        for one in self.second(t):
            one.start()

    def own_block(self, t):
        slot = lax.rem(t, SLOTS)
        for one in self.second(t):
            one.wait_recv()
        total = wide_sum(self.g[slot, self.rows(self.chip), :], self.half[lax.rem(t, HALF_SLOTS), self.within(self.chip), :], self.far[0, lax.rem(t, RING_SLOTS)], self.far[1, lax.rem(t, RING_SLOTS)]).astype(BF16)
        self.own[t] = total
        wide = total.astype(F32)
        self.squares[...] += jnp.sum((wide * wide).reshape(-1, 8, 128), axis=0)

        @pl.when(t < self.gathered)
        def _():
            self.kept(t).start()
            for one in self.spread(t):
                one.start()

        @pl.when((t >= self.gathered) & (t < self.split))
        def _():
            self.kept_alone(t, 0).start()

        @pl.when(t >= self.split)
        def _():
            self.kept_alone(t, 1).start()

        for one in (self.swap(t), *self.first(t), *self.second(t)):
            one.wait_send()

    def forward_near(self, t):
        right, left, _ = self.spread(t)
        right.wait_recv()
        left.wait_recv()
        for one in (*self.onward(t), *self.across_chip(t)):
            one.start()

    def forward_far(self, t):
        for one in self.onward(t):
            one.wait_recv()
        self.last(t).start()

    def finish(self, t):
        self.kept(t).wait()
        right, left, other = self.spread(t)
        other.wait_recv()
        for one in self.across_chip(t):
            one.wait_recv()
        self.last(t).wait_recv()
        for one in (right, left, other, *self.onward(t), *self.across_chip(t), self.last(t)):
            one.wait_send()


def greet(everyone):
    chips, chip, core, right, left, _ = place()
    barrier = pltpu.get_barrier_semaphore()
    if everyone:
        me = lax.axis_index("dp")
        others = [lax.rem(me + k, 2 * chips) for k in range(1, 2 * chips)]
    else:
        others = [right * 2 + core, left * 2 + core, chip * 2 + 1 - core]
    for other in others:
        pl.semaphore_signal(barrier, inc=1, device_id={"dp": other}, device_id_type=MESH)
    pl.semaphore_wait(barrier, len(others))


def tile_gradients(g, slot, at, dyt, dgate, dup, act):
    g[slot, :, 0:TILE] = nn(at[...], dgate[...]).astype(BF16)
    g[slot, :, TILE : 2 * TILE] = nn(at[...], dup[...]).astype(BF16)
    g[slot, :, 2 * TILE : 3 * TILE] = nn(dyt[...], act[...]).astype(BF16)


def activations(gate, up, d, act, dgate, dup, r):
    s = sigmoid(gate)
    silu = gate * s
    act[r, :] = (silu * up).astype(BF16)
    d_up = (d * silu).astype(BF16)
    d_gate = (d * up * (s + silu * (1.0 - s))).astype(BF16)
    dup[r, :] = d_up
    dgate[r, :] = d_gate
    return d_gate, d_up


def backward_kernel(tiles, left, count, h_ref, dy_ref, at_ref, gate_ref, up_ref, wg_ref, wu_ref, wd_ref, all_ref, own_one_ref, own_two_ref, factor_ref,
                    a, at, dyt, act, dgate, dup, wide, wg, wu, wd, loaded, all_squares, sent, arrived, *comm):
    j = pl.program_id(0)
    d = h_ref.shape[1]
    tokens = h_ref.shape[0]
    exchange = Exchange(2 * tiles, tiles, all_ref, (own_one_ref, own_two_ref), *comm)
    at_end = (j == tiles - 1) | (j == 2 * tiles - 1)
    acc = wide.at[:, 0:d]

    def saved(i):
        cols = pl.ds(pl.multiple_of(i * TILE, 128), TILE)
        return (
            pltpu.make_async_copy(gate_ref.at[:, cols], wide.at[:, 0:TILE], loaded.at[0]),
            pltpu.make_async_copy(up_ref.at[:, cols], wide.at[:, TILE : 2 * TILE], loaded.at[1]),
        )

    @pl.when(j == 0)
    def _():
        greet(True)
        exchange.squares[...] = jnp.zeros_like(exchange.squares)

        def norm(c, _):
            r = rows_of(c)
            x = h_ref[r, :].astype(F32)
            normed = (x * scale_of(x)).astype(BF16)
            at[:, r] = normed.T
            dyt[:, r] = dy_ref[r, :].T
            a[r, :] = normed
            acc[r, :] = jnp.zeros((CHUNK, d), F32)
            return _
        lax.fori_loop(0, tokens // CHUNK, norm, 0)

    @pl.when(j < tiles)
    def _():
        hold(wg_ref, wg, 1, left, at_end)
        hold(wu_ref, wu, 1, left, at_end)
        hold(wd_ref, wd, 0, left, at_end)

        def body(c, _):
            r = rows_of(c)
            gate = nn(a[r, :], wg[...])
            up = nn(a[r, :], wu[...])
            d = nt(dy_ref[r, :], wd[...]).astype(BF16).astype(F32)
            d_gate, d_up = activations(gate, up, d, act, dgate, dup, r)
            acc[r, :] += nt(d_gate, wg[...]) + nt(d_up, wu[...])

            @pl.when(c == 0)
            def _():
                exchange.early(j)

            @pl.when(c == 1)
            def _():
                exchange.midway(j)

            return 0
        lax.fori_loop(0, tokens // CHUNK, body, 0)

    @pl.when(j == tiles)
    def _():
        normed = pltpu.make_async_copy(at_ref, at, loaded.at[2])
        normed.start()

        def out(c, _):
            r = rows_of(c)
            x = h_ref[r, :].astype(F32)
            scale = scale_of(x)
            da = acc[r, :].astype(BF16).astype(F32)
            dot = jnp.mean(da * x, -1, keepdims=True)
            by = scale * da - x * (scale * scale * scale * dot)
            dh = (dy_ref[r, :].astype(F32) + by.astype(BF16).astype(F32)).astype(BF16)
            a[r, :] = dh
            dyt[:, r] = dh.T
            return _
        lax.fori_loop(0, tokens // CHUNK, out, 0)
        for one in saved(0):
            one.start()
        normed.wait()

    @pl.when((j >= tiles) & (j < 2 * tiles))
    def _():
        hold(wd_ref, wd, 0, left, at_end)
        for one in saved(j - tiles):
            one.wait()
        for c in range(tokens // WIDE):
            r = pl.ds(c * WIDE, WIDE)
            d = nt(a[r, :], wd[...]).astype(BF16).astype(F32)
            activations(wide[r, 0:TILE], wide[r, TILE : 2 * TILE], d, act, dgate, dup, r)

        @pl.when(j < 2 * tiles - 1)
        def _():
            for one in saved(j - tiles + 1):
                one.start()

    @pl.when(j >= tiles)
    def _():
        exchange.early(j)

    @pl.when(j < 2 * tiles)
    def _():
        tile_gradients(exchange.g, lax.rem(j, SLOTS), at, dyt, dgate, dup, act)

    exchange.late(j)

    @pl.when(j == pl.num_programs(0) - 1)
    def _():
        me = lax.axis_index("dp")
        n = lax.axis_size("dp")
        all_squares[me] = exchange.squares[...]
        copies = [
            pltpu.make_async_remote_copy(
                src_ref=exchange.squares, dst_ref=all_squares.at[me], send_sem=sent.at[k], recv_sem=arrived.at[k],
                device_id={"dp": lax.rem(me + k, n)}, device_id_type=MESH,
            )
            for k in range(1, n)
        ]
        for one in copies:
            one.start()
        for one in copies:
            one.wait()
        mean = jnp.sum(all_squares[...]) / count
        factor_ref[...] = jnp.full(factor_ref.shape, jnp.minimum(1.0, 0.5 * lax.rsqrt(mean + 1e-30)), F32)


def whole(shape):
    return pl.BlockSpec(shape, lambda j: (0,) * len(shape), pipeline_mode=pl.Buffered(1))


def params():
    return pltpu.CompilerParams(dimension_semantics=("arbitrary",), vmem_limit_bytes=62 * 1024 * 1024)


def forward(x, w, layer):
    tokens, d = x.shape
    ff = w[0].shape[2]
    tiles = pl.cdiv(ff, TILE)
    col = pl.BlockSpec((1, d, TILE), lambda j: (layer, 0, j))
    row = pl.BlockSpec((1, TILE, d), lambda j: (layer, j, 0))
    saved = pl.BlockSpec((tokens, TILE), lambda j: (0, j))
    return pl.pallas_call(
        functools.partial(forward_kernel, tokens // CHUNK, ff - (tiles - 1) * TILE),
        grid=(tiles,),
        in_specs=[whole((tokens, d)), col, col, row],
        out_specs=[whole((tokens, d)), whole((d, tokens)), saved, saved],
        out_shape=[jax.ShapeDtypeStruct((tokens, d), BF16), jax.ShapeDtypeStruct((d, tokens), BF16)] + [jax.ShapeDtypeStruct((tokens, tiles * TILE), F32)] * 2,
        scratch_shapes=[pltpu.VMEM((tokens, d), BF16), pltpu.VMEM((tokens, d), F32), pltpu.VMEM((d, TILE), BF16), pltpu.VMEM((d, TILE), BF16), pltpu.VMEM((TILE, d), BF16)],
        compiler_params=params(),
        cost_estimate=pl.CostEstimate(flops=6 * tokens * d * ff, bytes_accessed=8 * tokens * ff, transcendentals=tokens * ff),
        name="forward",
    )(x, *w)


def backward(h, dy, at, gate, up, w, n, count):
    tokens, d = h.shape
    ff = w[0].shape[2]
    tiles = pl.cdiv(ff, TILE)
    width, depth = 3 * TILE, d // n

    def late(j):
        return jnp.where(j < tiles, 1, 0)

    def tile(j):
        return jnp.minimum(jnp.where(j < tiles, j, j - tiles), tiles - 1)

    col = pl.BlockSpec((1, d, TILE), lambda j: (1, 0, jnp.minimum(j, tiles - 1)))
    row = pl.BlockSpec((1, TILE, d), lambda j: (late(j), tile(j), 0))
    hbm = pl.BlockSpec(memory_space=pl.ANY)
    return pl.pallas_call(
        functools.partial(backward_kernel, tiles, ff - (tiles - 1) * TILE, count),
        grid=(2 * tiles + 4,),
        in_specs=[whole((tokens, d)), whole((tokens, d)), hbm, hbm, hbm, col, col, row],
        out_specs=[hbm, hbm, hbm, whole((8, 128))],
        out_shape=[
            jax.ShapeDtypeStruct((d, width * tiles), BF16),
            jax.ShapeDtypeStruct((depth, width * (tiles - 3)), BF16),
            jax.ShapeDtypeStruct((depth, width * 3), BF16),
            jax.ShapeDtypeStruct((8, 128), F32),
        ],
        scratch_shapes=[
            pltpu.VMEM((tokens, d), BF16),
            pltpu.VMEM((d, tokens), BF16),
            pltpu.VMEM((d, tokens), BF16),
            pltpu.VMEM((tokens, TILE), BF16),
            pltpu.VMEM((tokens, TILE), BF16),
            pltpu.VMEM((tokens, TILE), BF16),
            pltpu.VMEM((tokens, 2 * TILE), F32),
            pltpu.VMEM((d, TILE), BF16),
            pltpu.VMEM((d, TILE), BF16),
            pltpu.VMEM((TILE, d), BF16),
            pltpu.SemaphoreType.DMA((3,)),
            pltpu.VMEM((n, 8, 128), F32),
            pltpu.SemaphoreType.DMA((n,)),
            pltpu.SemaphoreType.DMA((n,)),
            pltpu.VMEM((SLOTS, d, width), BF16),
            pltpu.VMEM((HALF_SLOTS, d // 2, width), BF16),
            pltpu.VMEM((2, RING_SLOTS, depth, width // 2), BF16),
            pltpu.VMEM((2, RING_SLOTS, depth, width), BF16),
            pltpu.VMEM((2 * tiles, depth, width), BF16),
            pltpu.VMEM((8, 128), F32),
            pltpu.SemaphoreType.DMA((13, 2 * tiles)),
            pltpu.SemaphoreType.DMA((13, 2 * tiles)),
            pltpu.SemaphoreType.DMA((2 * tiles,)),
        ],
        compiler_params=pltpu.CompilerParams(
            dimension_semantics=("arbitrary",), vmem_limit_bytes=67_000_000, collective_id=0, has_side_effects=True
        ),
        cost_estimate=pl.CostEstimate(flops=24 * tokens * d * ff, bytes_accessed=8 * tokens * ff, transcendentals=2 * tokens * ff),
        name="backward",
    )(h, dy, at, gate, up, *w)


def adamw_kernel(fresh, cores, factor_ref, g_ref, *refs):
    nine, outs = refs[:9], refs[9:] if fresh else refs[18:]
    factor = factor_ref[0, 0]
    n = ROWS if cores is None else cores[0] * cores[1]
    depth = g_ref.shape[0] // n

    def block(b):
        return b if cores is None else b % cores[1] * cores[0] + b // cores[1]

    def one(i, g, r):
        m = 0.9 * nine[3 + i][0, r, :] + 0.1 * g
        v = 0.95 * nine[6 + i][0, r, :] + 0.05 * g * g
        w = nine[i][0, r, :].astype(F32)
        outs[i][0, r, :] = (w - 0.02 * (m * lax.rsqrt(v + 1e-8) + 0.1 * w)).astype(BF16)
        outs[3 + i][0, r, :] = m
        outs[6 + i][0, r, :] = v

    def along(b, _):
        r = pl.ds(pl.multiple_of(b * depth, 16), depth)
        source = pl.ds(pl.multiple_of(block(b) * depth, 16), depth)
        for i in range(2):
            one(i, g_ref[source, i * TILE : (i + 1) * TILE].astype(F32) * factor, r)
        return 0
    lax.fori_loop(0, n, along, 0)

    def across(c, _):
        r = pl.ds(pl.multiple_of(c * 128, 128), 128)
        cols = pl.ds(pl.multiple_of(2 * TILE + c * 128, 128), 128)
        if cores is None:
            g = g_ref[:, cols]
        else:
            g = jnp.concatenate([g_ref[pl.ds(block(b) * depth, depth), cols] for b in range(n)])
        one(2, (g.astype(F32) * factor).T, r)
        return 0
    lax.fori_loop(0, TILE // 128, across, 0)


def adamw(factor, g, w, m, v, layer, first, last, cores=None, so_far=None):
    layers, d, ff = w[0].shape
    count = last - first
    col = pl.BlockSpec((1, d, TILE), lambda j: (layer, 0, j + first))
    row = pl.BlockSpec((1, TILE, d), lambda j: (layer, j + first, 0))
    nine = [col, col, row] * 3
    arrays = [*w, *m, *v]
    held = [] if so_far is None else list(so_far)
    return pl.pallas_call(
        functools.partial(adamw_kernel, so_far is None, cores),
        grid=(count,),
        in_specs=[pl.BlockSpec(memory_space=pltpu.SMEM), pl.BlockSpec((d, 3 * TILE), lambda j: (0, j))] + nine + [pl.BlockSpec(memory_space=pl.ANY)] * len(held),
        out_specs=nine,
        out_shape=[jax.ShapeDtypeStruct(a.shape, a.dtype) for a in arrays],
        input_output_aliases={11 + i: i for i in range(len(held))},
        compiler_params=params(),
        cost_estimate=pl.CostEstimate(flops=60 * d * TILE * count, bytes_accessed=66 * d * TILE * count, transcendentals=3 * d * TILE * count),
        name="adamw",
    )(factor, g, *arrays, *held)


def solution(mesh):
    n = mesh.shape["dp"]

    def step(x, dy, *arrays):
        w, m, v = (arrays[i : i + 3] for i in (0, 3, 6))
        x, dy = x[0], dy[0]
        h, at, gate, up = forward(x, w, 0)
        g1, *blocks, factor = backward(h, dy, at, gate, up, w, n, sum(a.size for a in w))
        tiles = pl.cdiv(w[0].shape[2], TILE)
        parts = [(0, tiles - 3), (tiles - 3, tiles)]
        pieces = [lax.all_gather(s0, "dp", axis=0, tiled=True) for s0 in blocks]
        new = adamw(factor, g1, w, m, v, 1, 0, tiles)
        for (first, last), g0 in zip(parts, pieces, strict=True):
            new = adamw(factor, g0, w, m, v, 0, first, last, (2, n // 2), new)
        return tuple(new)

    return jax.shard_map(
        step,
        mesh=mesh,
        in_specs=(P(("rep", "dp"), None, None),) * 2 + (P(None, None, None),) * 9,
        out_specs=(P("rep", None, None),) * 9,
        check_vma=False,
    )
```

```python
import functools
import jax
import jax.numpy as jnp
from jax import lax
from jax.experimental import pallas as pl
from jax.experimental.pallas import tpu as pltpu
from jax.sharding import PartitionSpec as P

F32, BF16 = jnp.float32, jnp.bfloat16
TILE = 512
CHUNK = 1024
WIDE = 2048
SLOTS, HALF_SLOTS, RING_SLOTS = 4, 6, 4
ROWS = 8
MESH = pl.DeviceIdType.MESH


def nn(a, b):
    return jnp.dot(a, b, preferred_element_type=F32)


def nt(a, b):
    return lax.dot_general(a, b, (((1,), (1,)), ((), ())), preferred_element_type=F32)


def scale_of(wide):
    return lax.rsqrt(jnp.mean(wide * wide, -1, keepdims=True) + 1e-6)


def sigmoid(x):
    return 0.5 * jnp.tanh(0.5 * x) + 0.5


def rows_of(c):
    return pl.ds(pl.multiple_of(c * CHUNK, CHUNK), CHUNK)


def hold(ref, kept, axis, left, at_end):
    kept[...] = ref[0]
    if left < TILE:
        @pl.when(at_end)
        def _():
            if axis == 1:
                kept[:, left:] = jnp.zeros((kept.shape[0], TILE - left), kept.dtype)
            else:
                kept[left:, :] = jnp.zeros((TILE - left, kept.shape[1]), kept.dtype)


def forward_kernel(chunks, left, x_ref, wg_ref, wu_ref, wd_ref, h_ref, at_ref, gate_ref, up_ref, a, acc, wg, wu, wd):
    j = pl.program_id(0)

    @pl.when(j == 0)
    def _():
        def norm(c, _):
            wide = x_ref[rows_of(c), :].astype(F32)
            normed = (wide * scale_of(wide)).astype(BF16)
            a[rows_of(c), :] = normed
            at_ref[:, rows_of(c)] = normed.T
            acc[rows_of(c), :] = jnp.zeros((CHUNK, acc.shape[1]), F32)
            return _
        lax.fori_loop(0, chunks, norm, 0)

    hold(wg_ref, wg, 1, left, j == pl.num_programs(0) - 1)
    hold(wu_ref, wu, 1, left, j == pl.num_programs(0) - 1)
    hold(wd_ref, wd, 0, left, j == pl.num_programs(0) - 1)

    def body(c, _):
        r = rows_of(c)
        gate = nn(a[r, :], wg[...])
        up = nn(a[r, :], wu[...])
        gate_ref[r, :] = gate
        up_ref[r, :] = up
        act = (gate * sigmoid(gate) * up).astype(BF16)
        acc[r, :] += nn(act, wd[...])
        return _
    lax.fori_loop(0, chunks, body, 0)

    @pl.when(j == pl.num_programs(0) - 1)
    def _():
        def out(c, _):
            r = rows_of(c)
            h_ref[r, :] = (x_ref[r, :].astype(F32) + acc[r, :].astype(BF16).astype(F32)).astype(BF16)
            return _
        lax.fori_loop(0, chunks, out, 0)


def place():
    chips = lax.axis_size("dp") // 2
    me = lax.axis_index("dp")
    chip, core = me // 2, lax.rem(me, 2)
    right, left = lax.rem(chip + 1, chips), lax.rem(chip + chips - 1, chips)
    return chips, chip, core, right, left, lax.rem(chip + 2, chips)


def wide_sum(*terms):
    total = terms[0].astype(F32)
    for term in terms[1:]:
        total = total + term.astype(F32)
    return total


class Exchange:
    def __init__(self, tiles, gathered, all_ref, own_ref, g, half, near, far, own, squares, send, recv, local):
        self.tiles, self.gathered, self.all_ref, self.own_ref = tiles, gathered, all_ref, own_ref
        self.g, self.half, self.near, self.far, self.own, self.squares = g, half, near, far, own, squares
        self.send, self.recv, self.local = send, recv, local
        self.chips, self.chip, self.core, self.right, self.left, self.across = place()
        self.depth, self.width = own.shape[1], own.shape[2]
        self.mid = self.width // 2
        self.split = gathered + own_ref[0].shape[1] // self.width

    def copy(self, kind, t, src, dst, chip=None, core=None):
        to = (self.chip if chip is None else chip) * 2 + (self.core if core is None else core)
        return pltpu.make_async_remote_copy(
            src_ref=src, dst_ref=dst, send_sem=self.send.at[kind, t], recv_sem=self.recv.at[kind, t], device_id={"dp": to}, device_id_type=MESH
        )

    def rows(self, chip, core=None):
        core = self.core if core is None else core
        return pl.ds(pl.multiple_of((core * self.chips + chip) * self.depth, 16), self.depth)

    def within(self, chip):
        return pl.ds(pl.multiple_of(chip * self.depth, 16), self.depth)

    def swap(self, t):
        theirs = pl.ds(pl.multiple_of((1 - self.core) * self.chips * self.depth, 16), self.chips * self.depth)
        return self.copy(0, t, self.g.at[lax.rem(t, SLOTS), theirs, :], self.half.at[lax.rem(t, HALF_SLOTS)], core=1 - self.core)

    def first(self, t):
        slot, r = lax.rem(t, SLOTS), self.rows(self.across)
        return (
            self.copy(1, t, self.g.at[slot, r, pl.ds(0, self.mid)], self.near.at[0, lax.rem(t, RING_SLOTS)], chip=self.right),
            self.copy(2, t, self.g.at[slot, r, pl.ds(self.mid, self.mid)], self.near.at[1, lax.rem(t, RING_SLOTS)], chip=self.left),
        )

    def second(self, t):
        slot = lax.rem(t, SLOTS)
        return (
            self.copy(3, t, self.g.at[slot, self.rows(self.right), :], self.far.at[0, lax.rem(t, RING_SLOTS)], chip=self.right),
            self.copy(4, t, self.g.at[slot, self.rows(self.left), :], self.far.at[1, lax.rem(t, RING_SLOTS)], chip=self.left),
        )

    def cols(self, t, start=0, size=None):
        return pl.ds(pl.multiple_of(t * self.width + start, 128), self.width if size is None else size)

    def region(self, chip, t, start=0, size=None):
        return self.all_ref.at[self.rows(chip), self.cols(t, start, size)]

    def spread(self, t):
        there = self.region(self.chip, t)
        return (
            self.copy(5, t, self.own.at[t], there, chip=self.right),
            self.copy(6, t, self.own.at[t], there, chip=self.left),
            self.copy(7, t, self.own.at[t], there, core=1 - self.core),
        )

    def onward(self, t):
        one, two = self.region(self.left, t, 0, self.mid), self.region(self.right, t, self.mid, self.mid)
        return (self.copy(8, t, one, one, chip=self.right), self.copy(9, t, two, two, chip=self.left))

    def across_chip(self, t):
        one, two = self.region(self.left, t), self.region(self.right, t)
        return (self.copy(10, t, one, one, core=1 - self.core), self.copy(11, t, two, two, core=1 - self.core))

    def last(self, t):
        it = self.region(self.across, t)
        return self.copy(12, t, it, it, core=1 - self.core)

    def kept(self, t):
        return pltpu.make_async_copy(self.own.at[t], self.region(self.chip, t), self.local.at[t])

    def kept_alone(self, t, part):
        ref = self.own_ref[part]
        start = self.gathered if part == 0 else self.split
        return pltpu.make_async_copy(self.own.at[t], ref.at[:, self.cols(t - start)], self.local.at[t])

    def stage(self, j, lag, what, start, stop):
        t = j - lag

        @pl.when((t >= start) & (t < stop))
        def _():
            what(t)

    def early(self, j):
        soon = self.gathered - 1
        self.stage(j, 1, self.far_block, 0, self.tiles)
        self.stage(j, 2, self.neighbours, soon, self.tiles)
        self.stage(j, 2, self.own_block, 0, soon)
        self.stage(j, 3, self.forward_far, 0, soon - 1)

    def midway(self, j):
        self.stage(j, 1, self.neighbours, 0, self.gathered - 1)

    def late(self, j):
        soon = self.gathered - 1
        self.stage(j, 0, lambda t: self.swap(t).start(), 0, self.tiles)
        self.stage(j, 3, self.own_block, soon, self.tiles)
        self.stage(j, 4, lambda t: self.kept_alone(t, 0).wait(), self.gathered, self.split)
        self.stage(j, 4, lambda t: self.kept_alone(t, 1).wait(), self.split, self.tiles)
        self.stage(j, 3, self.finish, 0, soon - 1)
        self.stage(j, 2, self.forward_near, 0, soon - 1)
        for t, lag in ((soon - 1, 3), (soon, 4)):
            self.stage(j, lag, self.forward_near, t, t + 1)
            self.stage(j, lag + 1, self.forward_far, t, t + 1)
            self.stage(j, lag + 2, self.finish, t, t + 1)

    def far_block(self, t):
        self.swap(t).wait_recv()
        slot, r = lax.rem(t, SLOTS), self.rows(self.across)
        self.g[slot, r, :] = wide_sum(self.g[slot, r, :], self.half[lax.rem(t, HALF_SLOTS), self.within(self.across), :]).astype(BF16)
        for one in self.first(t):
            one.start()

    def neighbours(self, t):
        slot, mid = lax.rem(t, SLOTS), self.mid
        for one in self.first(t):
            one.wait_recv()
        for chip, side in ((self.right, 0), (self.left, 1)):
            r, h = self.rows(chip), self.within(chip)
            met, other = pl.ds(side * mid, mid), pl.ds((1 - side) * mid, mid)
            self.g[slot, r, met] = wide_sum(self.g[slot, r, met], self.half[lax.rem(t, HALF_SLOTS), h, met], self.near[side, lax.rem(t, RING_SLOTS)]).astype(BF16)
            self.g[slot, r, other] = wide_sum(self.g[slot, r, other], self.half[lax.rem(t, HALF_SLOTS), h, other]).astype(BF16)
        for one in self.second(t):
            one.start()

    def own_block(self, t):
        slot = lax.rem(t, SLOTS)
        for one in self.second(t):
            one.wait_recv()
        total = wide_sum(self.g[slot, self.rows(self.chip), :], self.half[lax.rem(t, HALF_SLOTS), self.within(self.chip), :], self.far[0, lax.rem(t, RING_SLOTS)], self.far[1, lax.rem(t, RING_SLOTS)]).astype(BF16)
        self.own[t] = total
        wide = total.astype(F32)
        self.squares[...] += jnp.sum((wide * wide).reshape(-1, 8, 128), axis=0)

        @pl.when(t < self.gathered)
        def _():
            self.kept(t).start()
            for one in self.spread(t):
                one.start()

        @pl.when((t >= self.gathered) & (t < self.split))
        def _():
            self.kept_alone(t, 0).start()

        @pl.when(t >= self.split)
        def _():
            self.kept_alone(t, 1).start()

        for one in (self.swap(t), *self.first(t), *self.second(t)):
            one.wait_send()

    def forward_near(self, t):
        right, left, _ = self.spread(t)
        right.wait_recv()
        left.wait_recv()
        for one in (*self.onward(t), *self.across_chip(t)):
            one.start()

    def forward_far(self, t):
        for one in self.onward(t):
            one.wait_recv()
        self.last(t).start()

    def finish(self, t):
        self.kept(t).wait()
        right, left, other = self.spread(t)
        other.wait_recv()
        for one in self.across_chip(t):
            one.wait_recv()
        self.last(t).wait_recv()
        for one in (right, left, other, *self.onward(t), *self.across_chip(t), self.last(t)):
            one.wait_send()


def greet(everyone):
    chips, chip, core, right, left, _ = place()
    barrier = pltpu.get_barrier_semaphore()
    if everyone:
        me = lax.axis_index("dp")
        others = [lax.rem(me + k, 2 * chips) for k in range(1, 2 * chips)]
    else:
        others = [right * 2 + core, left * 2 + core, chip * 2 + 1 - core]
    for other in others:
        pl.semaphore_signal(barrier, inc=1, device_id={"dp": other}, device_id_type=MESH)
    pl.semaphore_wait(barrier, len(others))


def tile_gradients(g, slot, at, dyt, dgate, dup, act):
    g[slot, :, 0:TILE] = nn(at[...], dgate[...]).astype(BF16)
    g[slot, :, TILE : 2 * TILE] = nn(at[...], dup[...]).astype(BF16)
    g[slot, :, 2 * TILE : 3 * TILE] = nn(dyt[...], act[...]).astype(BF16)


def activations(gate, up, d, act, dgate, dup, r):
    s = sigmoid(gate)
    silu = gate * s
    act[r, :] = (silu * up).astype(BF16)
    d_up = (d * silu).astype(BF16)
    d_gate = (d * up * (s + silu * (1.0 - s))).astype(BF16)
    dup[r, :] = d_up
    dgate[r, :] = d_gate
    return d_gate, d_up


def backward_kernel(tiles, left, count, h_ref, dy_ref, at_ref, gate_ref, up_ref, wg_ref, wu_ref, wd_ref, all_ref, own_one_ref, own_two_ref, factor_ref,
                    a, at, dyt, act, dgate, dup, wide, wg, wu, wd, loaded, all_squares, sent, arrived, *comm):
    j = pl.program_id(0)
    d = h_ref.shape[1]
    tokens = h_ref.shape[0]
    exchange = Exchange(2 * tiles, tiles, all_ref, (own_one_ref, own_two_ref), *comm)
    at_end = (j == tiles - 1) | (j == 2 * tiles - 1)
    acc = wide.at[:, 0:d]

    def saved(i):
        cols = pl.ds(pl.multiple_of(i * TILE, 128), TILE)
        return (
            pltpu.make_async_copy(gate_ref.at[:, cols], wide.at[:, 0:TILE], loaded.at[0]),
            pltpu.make_async_copy(up_ref.at[:, cols], wide.at[:, TILE : 2 * TILE], loaded.at[1]),
        )

    @pl.when(j == 0)
    def _():
        greet(True)
        exchange.squares[...] = jnp.zeros_like(exchange.squares)

        def norm(c, _):
            r = rows_of(c)
            x = h_ref[r, :].astype(F32)
            normed = (x * scale_of(x)).astype(BF16)
            at[:, r] = normed.T
            dyt[:, r] = dy_ref[r, :].T
            a[r, :] = normed
            acc[r, :] = jnp.zeros((CHUNK, d), F32)
            return _
        lax.fori_loop(0, tokens // CHUNK, norm, 0)

    @pl.when(j < tiles)
    def _():
        hold(wg_ref, wg, 1, left, at_end)
        hold(wu_ref, wu, 1, left, at_end)
        hold(wd_ref, wd, 0, left, at_end)

        def body(c, _):
            r = rows_of(c)
            gate = nn(a[r, :], wg[...])
            up = nn(a[r, :], wu[...])
            d = nt(dy_ref[r, :], wd[...]).astype(BF16).astype(F32)
            d_gate, d_up = activations(gate, up, d, act, dgate, dup, r)
            acc[r, :] += nt(d_gate, wg[...]) + nt(d_up, wu[...])

            @pl.when(c == 0)
            def _():
                exchange.early(j)

            @pl.when(c == 1)
            def _():
                exchange.midway(j)

            return 0
        lax.fori_loop(0, tokens // CHUNK, body, 0)

    @pl.when(j == tiles)
    def _():
        normed = pltpu.make_async_copy(at_ref, at, loaded.at[2])
        normed.start()

        def out(c, _):
            r = rows_of(c)
            x = h_ref[r, :].astype(F32)
            scale = scale_of(x)
            da = acc[r, :].astype(BF16).astype(F32)
            dot = jnp.mean(da * x, -1, keepdims=True)
            by = scale * da - x * (scale * scale * scale * dot)
            dh = (dy_ref[r, :].astype(F32) + by.astype(BF16).astype(F32)).astype(BF16)
            a[r, :] = dh
            dyt[:, r] = dh.T
            return _
        lax.fori_loop(0, tokens // CHUNK, out, 0)
        for one in saved(0):
            one.start()
        normed.wait()

    @pl.when((j >= tiles) & (j < 2 * tiles))
    def _():
        hold(wd_ref, wd, 0, left, at_end)
        for one in saved(j - tiles):
            one.wait()
        for c in range(tokens // WIDE):
            r = pl.ds(c * WIDE, WIDE)
            d = nt(a[r, :], wd[...]).astype(BF16).astype(F32)
            activations(wide[r, 0:TILE], wide[r, TILE : 2 * TILE], d, act, dgate, dup, r)

        @pl.when(j < 2 * tiles - 1)
        def _():
            for one in saved(j - tiles + 1):
                one.start()

    @pl.when(j >= tiles)
    def _():
        exchange.early(j)

    @pl.when(j < 2 * tiles)
    def _():
        tile_gradients(exchange.g, lax.rem(j, SLOTS), at, dyt, dgate, dup, act)

    exchange.late(j)

    @pl.when(j == pl.num_programs(0) - 1)
    def _():
        me = lax.axis_index("dp")
        n = lax.axis_size("dp")
        all_squares[me] = exchange.squares[...]
        copies = [
            pltpu.make_async_remote_copy(
                src_ref=exchange.squares, dst_ref=all_squares.at[me], send_sem=sent.at[k], recv_sem=arrived.at[k],
                device_id={"dp": lax.rem(me + k, n)}, device_id_type=MESH,
            )
            for k in range(1, n)
        ]
        for one in copies:
            one.start()
        for one in copies:
            one.wait()
        mean = jnp.sum(all_squares[...]) / count
        factor_ref[...] = jnp.full(factor_ref.shape, jnp.minimum(1.0, 0.5 * lax.rsqrt(mean + 1e-30)), F32)


def whole(shape):
    return pl.BlockSpec(shape, lambda j: (0,) * len(shape), pipeline_mode=pl.Buffered(1))


def params():
    return pltpu.CompilerParams(dimension_semantics=("arbitrary",), vmem_limit_bytes=62 * 1024 * 1024)


def forward(x, w, layer):
    tokens, d = x.shape
    ff = w[0].shape[2]
    tiles = pl.cdiv(ff, TILE)
    col = pl.BlockSpec((1, d, TILE), lambda j: (layer, 0, j))
    row = pl.BlockSpec((1, TILE, d), lambda j: (layer, j, 0))
    saved = pl.BlockSpec((tokens, TILE), lambda j: (0, j))
    return pl.pallas_call(
        functools.partial(forward_kernel, tokens // CHUNK, ff - (tiles - 1) * TILE),
        grid=(tiles,),
        in_specs=[whole((tokens, d)), col, col, row],
        out_specs=[whole((tokens, d)), whole((d, tokens)), saved, saved],
        out_shape=[jax.ShapeDtypeStruct((tokens, d), BF16), jax.ShapeDtypeStruct((d, tokens), BF16)] + [jax.ShapeDtypeStruct((tokens, tiles * TILE), F32)] * 2,
        scratch_shapes=[pltpu.VMEM((tokens, d), BF16), pltpu.VMEM((tokens, d), F32), pltpu.VMEM((d, TILE), BF16), pltpu.VMEM((d, TILE), BF16), pltpu.VMEM((TILE, d), BF16)],
        compiler_params=pltpu.CompilerParams(
            dimension_semantics=("arbitrary",), vmem_limit_bytes=62 * 1024 * 1024
        ),
        cost_estimate=pl.CostEstimate(flops=6 * tokens * d * ff, bytes_accessed=8 * tokens * ff, transcendentals=tokens * ff),
        name="forward",
    )(x, *w)


def backward(h, dy, at, gate, up, w, n, count):
    tokens, d = h.shape
    ff = w[0].shape[2]
    tiles = pl.cdiv(ff, TILE)
    width, depth = 3 * TILE, d // n

    def late(j):
        return jnp.where(j < tiles, 1, 0)

    def tile(j):
        return jnp.minimum(jnp.where(j < tiles, j, j - tiles), tiles - 1)

    col = pl.BlockSpec((1, d, TILE), lambda j: (1, 0, jnp.minimum(j, tiles - 1)))
    row = pl.BlockSpec((1, TILE, d), lambda j: (late(j), tile(j), 0))
    hbm = pl.BlockSpec(memory_space=pl.ANY)
    return pl.pallas_call(
        functools.partial(backward_kernel, tiles, ff - (tiles - 1) * TILE, count),
        grid=(2 * tiles + 4,),
        in_specs=[whole((tokens, d)), whole((tokens, d)), hbm, hbm, hbm, col, col, row],
        out_specs=[hbm, hbm, hbm, whole((8, 128))],
        out_shape=[
            jax.ShapeDtypeStruct((d, width * tiles), BF16),
            jax.ShapeDtypeStruct((depth, width * (tiles - 3)), BF16),
            jax.ShapeDtypeStruct((depth, width * 3), BF16),
            jax.ShapeDtypeStruct((8, 128), F32),
        ],
        scratch_shapes=[
            pltpu.VMEM((tokens, d), BF16),
            pltpu.VMEM((d, tokens), BF16),
            pltpu.VMEM((d, tokens), BF16),
            pltpu.VMEM((tokens, TILE), BF16),
            pltpu.VMEM((tokens, TILE), BF16),
            pltpu.VMEM((tokens, TILE), BF16),
            pltpu.VMEM((tokens, 2 * TILE), F32),
            pltpu.VMEM((d, TILE), BF16),
            pltpu.VMEM((d, TILE), BF16),
            pltpu.VMEM((TILE, d), BF16),
            pltpu.SemaphoreType.DMA((3,)),
            pltpu.VMEM((n, 8, 128), F32),
            pltpu.SemaphoreType.DMA((n,)),
            pltpu.SemaphoreType.DMA((n,)),
            pltpu.VMEM((SLOTS, d, width), BF16),
            pltpu.VMEM((HALF_SLOTS, d // 2, width), BF16),
            pltpu.VMEM((2, RING_SLOTS, depth, width // 2), BF16),
            pltpu.VMEM((2, RING_SLOTS, depth, width), BF16),
            pltpu.VMEM((2 * tiles, depth, width), BF16),
            pltpu.VMEM((8, 128), F32),
            pltpu.SemaphoreType.DMA((13, 2 * tiles)),
            pltpu.SemaphoreType.DMA((13, 2 * tiles)),
            pltpu.SemaphoreType.DMA((2 * tiles,)),
        ],
        compiler_params=pltpu.CompilerParams(
            dimension_semantics=("arbitrary",), vmem_limit_bytes=67_000_000, collective_id=0, has_side_effects=True
        ),
        cost_estimate=pl.CostEstimate(flops=24 * tokens * d * ff, bytes_accessed=8 * tokens * ff, transcendentals=2 * tokens * ff),
        name="backward",
    )(h, dy, at, gate, up, *w)


def adamw_kernel(fresh, cores, factor_ref, g_ref, *refs):
    nine, outs = refs[:9], refs[9:] if fresh else refs[18:]
    factor = factor_ref[0, 0]
    n = ROWS if cores is None else cores[0] * cores[1]
    depth = g_ref.shape[0] // n

    def block(b):
        return b if cores is None else b % cores[1] * cores[0] + b // cores[1]

    def one(i, g, r):
        m = 0.9 * nine[3 + i][0, r, :] + 0.1 * g
        v = 0.95 * nine[6 + i][0, r, :] + 0.05 * g * g
        w = nine[i][0, r, :].astype(F32)
        outs[i][0, r, :] = (w - 0.02 * (m * lax.rsqrt(v + 1e-8) + 0.1 * w)).astype(BF16)
        outs[3 + i][0, r, :] = m
        outs[6 + i][0, r, :] = v

    def along(b, _):
        r = pl.ds(pl.multiple_of(b * depth, 16), depth)
        source = pl.ds(pl.multiple_of(block(b) * depth, 16), depth)
        for i in range(2):
            one(i, g_ref[source, i * TILE : (i + 1) * TILE].astype(F32) * factor, r)
        return 0
    lax.fori_loop(0, n, along, 0)

    def across(c, _):
        r = pl.ds(pl.multiple_of(c * 128, 128), 128)
        cols = pl.ds(pl.multiple_of(2 * TILE + c * 128, 128), 128)
        if cores is None:
            g = g_ref[:, cols]
        else:
            g = jnp.concatenate([g_ref[pl.ds(block(b) * depth, depth), cols] for b in range(n)])
        one(2, (g.astype(F32) * factor).T, r)
        return 0
    lax.fori_loop(0, TILE // 128, across, 0)


def adamw(factor, g, w, m, v, layer, first, last, cores=None, so_far=None):
    layers, d, ff = w[0].shape
    count = last - first
    col = pl.BlockSpec((1, d, TILE), lambda j: (layer, 0, j + first))
    row = pl.BlockSpec((1, TILE, d), lambda j: (layer, j + first, 0))
    nine = [col, col, row] * 3
    arrays = [*w, *m, *v]
    held = [] if so_far is None else list(so_far)
    return pl.pallas_call(
        functools.partial(adamw_kernel, so_far is None, cores),
        grid=(count,),
        in_specs=[pl.BlockSpec(memory_space=pltpu.SMEM), pl.BlockSpec((d, 3 * TILE), lambda j: (0, j))] + nine + [pl.BlockSpec(memory_space=pl.ANY)] * len(held),
        out_specs=nine,
        out_shape=[jax.ShapeDtypeStruct(a.shape, a.dtype) for a in arrays],
        input_output_aliases={11 + i: i for i in range(len(held))},
        compiler_params=params(),
        cost_estimate=pl.CostEstimate(flops=60 * d * TILE * count, bytes_accessed=66 * d * TILE * count, transcendentals=3 * d * TILE * count),
        name="adamw",
    )(factor, g, *arrays, *held)


def solution(mesh):
    n = mesh.shape["dp"]

    def step(x, dy, *arrays):
        w, m, v = (arrays[i : i + 3] for i in (0, 3, 6))
        x, dy = x[0], dy[0]
        h, at, gate, up = forward(x, w, 0)
        g1, *blocks, factor = backward(h, dy, at, gate, up, w, n, sum(a.size for a in w))
        tiles = pl.cdiv(w[0].shape[2], TILE)
        parts = [(0, tiles - 3), (tiles - 3, tiles)]
        pieces = [lax.all_gather(s0, "dp", axis=0, tiled=True) for s0 in blocks]
        new = adamw(factor, g1, w, m, v, 1, 0, tiles)
        for (first, last), g0 in zip(parts, pieces, strict=True):
            new = adamw(factor, g0, w, m, v, 0, first, last, (2, n // 2), new)
        return tuple(new)

    return jax.shard_map(
        step,
        mesh=mesh,
        in_specs=(P(("rep", "dp"), None, None),) * 2 + (P(None, None, None),) * 9,
        out_specs=(P("rep", None, None),) * 9,
        check_vma=False,
    )
```
